512 devices in a mesh: groups: 2 (over y), seq: 32 (over z), exp: 4 (over x), rep: 2 (over core).
Axes of the slice: x: 4, y: 2, z: 32, core: 2. Of those that a mesh axis runs over, the one named last changes fastest.
The devices are a block of a 4x8x32 slice.
Arguments:
- queries: bfloat16 [4096, 4096], P(('groups', 'seq'), ('exp', 'rep')), parts along dimension 0, may hold values from -4 to 4
- key_rows: bfloat16 [4096, 4096], P(('groups', 'seq'), ('exp', 'rep')), parts along dimension 0, may hold values from -4 to 4
- value_rows: bfloat16 [4096, 4096], P(('groups', 'seq'), ('exp', 'rep')), parts along dimension 0, may hold values from -6 to 6
- decay_log: float32 [4096, 32], P(('groups', 'seq'), ('exp', 'rep')), parts along dimension 0, may hold values from -1.5 to 0
- residual: bfloat16 [4096, 4096], P(('groups', 'seq'), ('exp', 'rep')), parts along dimension 0, may hold values from -6 to 6
- out_gate: bfloat16 [4096, 4096], P(('groups', 'seq'), ('exp', 'rep')), parts along dimension 0, may hold values from -6 to 6
- attn_gain: float32 [4096], P(('exp', 'rep')), may hold values from 0.1 to 1.9
- moe_gain: float32 [4096], P(('exp', 'rep')), may hold values from 0.1 to 1.9
- routes: int32 [4096, 2], P(('groups', 'seq')), parts along dimension 0, may hold values from 0 to 31, as said below
- route_weights: float32 [4096, 2], P(('groups', 'seq')), parts along dimension 0, may hold values from 0.3 to 1
- w_gate: bfloat16 [4, 4608, 4096], P('exp', 'seq'), may hold values from -0.09375 to 0.09375
- w_up: bfloat16 [4, 4608, 4096], P('exp', 'seq'), may hold values from -0.09375 to 0.09375
- w_down: bfloat16 [4, 4608, 4096], P('exp', 'seq'), may hold values from -0.09375 to 0.09375
Outputs:
- layer_out: bfloat16 [4096, 4096], P(('groups', 'seq'), ('exp', 'rep')), parts along dimension 0
The draws below stay inside these ranges and needn't reach their ends.
There are 2 independent parts, one for each index of `groups`. The reference program is written for one: setup_inputs(seed, part) draws one part's arguments, and reference() takes and returns one part's arrays. A program takes and returns all parts, laid end to end along the dimension named above; an argument that names none is the same for every part. Nothing has to cross between parts.
Inputs may be any that keep to these rules, and one draw needn't show every extreme that they name: `routes`: each row names two different experts. Within each aligned block of 64 rows no expert is named by more than 6 rows, every expert is named in every block, and one expert below 4 is named by exactly 6 rows in every block.
All inputs are finite; a program needn't handle non-finite values.
Results may differ from the reference program's by a relative error of at most 0.01.
Values may be sent and summed in bfloat16 or wider, within the bound.
No kernel may reach another device: no remote copies, remote signals or barrier semaphores. Data moves between devices by JAX's collectives and lax.ppermute only.
A program may use at most 64 MiB of HBM per device.

```python
from functools import partial
import jax
import jax.numpy as jnp
from jax import lax

HEAD = 128
HEAD_COUNT = 32
D = 4096
FF = 4608
ROUTED = 32
BLOCK = 64
EXPERTS = 4
CAP = 6
L = 2048
N_SEQ = 32
N_EXP = 4


def draw_routes(key, part):
    blocks = N_SEQ
    unit = BLOCK // ROUTED
    half_count = ROUTED // 2
    random_subkeys = jax.random.split(jax.random.fold_in(key, 11), 4)
    hot_expert = jax.random.randint(random_subkeys[0], (), 0, N_EXP)
    shifts = jax.random.randint(random_subkeys[1], (blocks, half_count), -unit, unit + 1)
    shifts = jnp.where(jnp.arange(half_count)[None, :] == hot_expert, unit, shifts)
    counts = jnp.concatenate([2 * unit + shifts, 2 * unit - shifts], axis=1)
    bounds = jnp.cumsum(counts, axis=1)
    places = jnp.arange(2 * BLOCK)
    sorted_ids = jnp.sum((bounds[:, None, :] <= places[None, :, None]).astype(jnp.int32), axis=2)

    def shuffle(block_key):
        return jax.random.permutation(block_key, BLOCK)
    orders = jax.vmap(shuffle)(jax.random.split(random_subkeys[2], blocks))
    first_ids = jnp.take_along_axis(sorted_ids, orders, axis=1)
    second_ids = jnp.take_along_axis(sorted_ids, orders + BLOCK, axis=1)
    flips = jax.random.randint(random_subkeys[3], (blocks, BLOCK), 0, 2)
    left_ids = jnp.where(flips == 1, second_ids, first_ids)
    right_ids = jnp.where(flips == 1, first_ids, second_ids)
    return jnp.stack([left_ids, right_ids], axis=2).reshape(blocks * BLOCK, 2).astype(jnp.int32)


def draw_decay_log(key, part):
    sequence_length = BLOCK * N_SEQ
    random_subkeys = jax.random.split(jax.random.fold_in(key, 23), 7)
    fast_share = 0.5
    fast_heads = jax.random.uniform(random_subkeys[0], (HEAD_COUNT,)) < fast_share
    fast_rate = jnp.exp(jax.random.uniform(random_subkeys[1], (HEAD_COUNT,), minval=jnp.log(1.0 / 50.0), maxval=jnp.log(1.0 / 30.0)))
    slow_rate = -jnp.log(jax.random.uniform(random_subkeys[2], (HEAD_COUNT,), minval=0.8, maxval=0.95)) / sequence_length
    rates = jnp.where(fast_heads, fast_rate, slow_rate)
    block_factor = jnp.repeat(jax.random.uniform(random_subkeys[3], (N_SEQ, HEAD_COUNT), minval=0.6, maxval=1.5), BLOCK, axis=0)
    token_factor = jax.random.uniform(random_subkeys[4], (sequence_length, HEAD_COUNT), minval=0.5, maxval=1.5)
    steady_portion = -rates[None, :] * block_factor * token_factor
    surge_position = jax.random.randint(random_subkeys[5], (2, HEAD_COUNT), 0, sequence_length)
    surge_length = jnp.log(jax.random.uniform(random_subkeys[6], (2, HEAD_COUNT), minval=0.5, maxval=0.8))
    token_positions = jnp.arange(sequence_length)[:, None]
    surge_events = jnp.where(token_positions == surge_position[0][None, :], surge_length[0][None, :], 0.0)
    surge_events = surge_events + jnp.where(token_positions == surge_position[1][None, :], surge_length[1][None, :], 0.0)
    return (steady_portion + surge_events).astype(jnp.float32)


def steps_of(stream_key, shape, cuts, least, largest):
    level = 1.0
    for position, blocks in cuts:
        heights = jax.random.uniform(jax.random.fold_in(jax.random.fold_in(stream_key, 6), position), (blocks,), jnp.float32, least / len(cuts), largest / len(cuts))
        level = level * jnp.repeat(jnp.exp(heights), shape[position] // blocks).reshape((-1,) + (1,) * (len(shape) - 1 - position))
    return level


def scatter_about(stream_key, shape, scale, limit, cuts=(), kind=jnp.bfloat16):
    drawn = scale * jax.random.normal(stream_key, shape, jnp.float32)
    if cuts:
        drawn = drawn * steps_of(stream_key, shape, cuts, -0.22, 0.18)
    return jnp.clip(drawn, -limit, limit).astype(kind)


def setup_inputs(seed: int = 0, part: int = 0) -> dict:
    key_of = jax.random.split(jax.random.key(seed), 14)
    own_keys = jax.random.split(jax.random.fold_in(key_of[13], part), 14)
    return {
        "queries": scatter_about(own_keys[0], (L, D), 0.3, 4.0, ((0, 32), (1, 8))),
        "key_rows": scatter_about(own_keys[1], (L, D), 0.3, 4.0, ((0, 32), (1, 8))),
        "value_rows": scatter_about(own_keys[2], (L, D), 1.0, 6.0, ((0, 32), (1, 8))),
        "decay_log": draw_decay_log(jax.random.fold_in(jax.random.fold_in(key_of[13], part), 71), part),
        "residual": scatter_about(own_keys[4], (L, D), 1.0, 6.0, ((0, 32), (1, 8))),
        "out_gate": scatter_about(own_keys[5], (L, D), 1.0, 6.0, ((0, 32), (1, 8))),
        "attn_gain": jnp.clip(1.0 + 0.18 * jax.random.normal(key_of[6], (D,), jnp.float32), 0.1, 1.9),
        "moe_gain": jnp.clip(1.0 + 0.18 * jax.random.normal(key_of[7], (D,), jnp.float32), 0.1, 1.9),
        "routes": draw_routes(jax.random.fold_in(jax.random.fold_in(key_of[13], part), 71), part),
        "route_weights": jnp.clip(0.3 + 0.7 * jax.random.uniform(own_keys[9], (L, 2), jnp.float32) ** steps_of(own_keys[9], (L, 2), ((0, 32),), -0.2, 0.2), 0.3, 1.0),
        "w_gate": scatter_about(key_of[10], (EXPERTS, FF, D), D ** -0.5, 0.09375, ((0, 4), (1, 32))),
        "w_up": scatter_about(key_of[11], (EXPERTS, FF, D), D ** -0.5, 0.09375, ((0, 4), (1, 32))),
        "w_down": scatter_about(key_of[12], (EXPERTS, FF, D), FF ** -0.5, 0.09375, ((0, 4), (1, 32))),
    }


EPSILON = 1e-06

def slot_tables(route_block, weight_block, experts, capacity):
    expert_ids = jnp.arange(experts, dtype=jnp.int32)
    onehot = (route_block[:, :, None] == expert_ids[None, None, :]).astype(jnp.int32)
    tokens = route_block.shape[0]
    flat_hits = onehot.reshape(tokens * 2, experts)
    before = jnp.cumsum(flat_hits, axis=0) - flat_hits
    places = jnp.arange(capacity, dtype=jnp.int32)
    hit_table = flat_hits[:, :, None] * (before[:, :, None] == places[None, None, :]).astype(jnp.int32)
    hit_table = hit_table.astype(jnp.float32).reshape(tokens, 2, experts * capacity)
    dispatch = lax.optimization_barrier(jnp.sum(hit_table, axis=1))
    combine = lax.optimization_barrier(jnp.sum(hit_table * weight_block[:, :, None], axis=1))
    return (dispatch, combine)

def block_attention(carried, inputs):
    query_blk, key_blk, value_blk, decay_blk = inputs
    cumulative = jnp.cumsum(decay_blk, axis=0)
    token_positions = jnp.arange(decay_blk.shape[0])
    causal = (token_positions[:, None] >= token_positions[None, :])[:, :, None]
    log_gaps = cumulative[:, None, :] - cumulative[None, :, :]
    decay_mask = jnp.where(causal, jnp.exp(jnp.where(causal, log_gaps, 0.0)), 0.0)
    scores = jnp.einsum('thd,jhd->htj', query_blk.astype(jnp.float32), key_blk.astype(jnp.float32))
    mixing = (scores * jnp.transpose(decay_mask, (2, 0, 1))).astype(jnp.bfloat16)
    local_part = jnp.einsum('htj,jhd->thd', mixing.astype(jnp.float32), value_blk.astype(jnp.float32))
    lifted = query_blk.astype(jnp.float32) * jnp.exp(cumulative)[:, :, None]
    carried_part = jnp.einsum('thd,hde->the', lifted, carried, precision=lax.Precision.HIGHEST)
    ending = cumulative[-1]
    faded_keys = key_blk.astype(jnp.float32) * jnp.exp(ending[None, :] - cumulative)[:, :, None]
    block_state = jnp.einsum('jhd,jhe->hde', faded_keys, value_blk.astype(jnp.float32), precision=lax.Precision.HIGHEST)
    updated = jnp.exp(ending)[:, None, None] * carried + block_state
    return (updated, local_part + carried_part)

def expert_apply(items):
    slot_rows, gate_mat, up_mat, down_mat = items
    gate_val = jnp.dot(slot_rows, jnp.transpose(gate_mat), preferred_element_type=jnp.float32)
    up_val = jnp.dot(slot_rows, jnp.transpose(up_mat), preferred_element_type=jnp.float32)
    inner_act = (jax.nn.silu(gate_val) * up_val).astype(jnp.bfloat16)
    row_count = slot_rows.shape[0]
    model_width = down_mat.shape[1]
    slab_width = down_mat.shape[0] // N_SEQ
    inner_slabs = jnp.transpose(inner_act.reshape(row_count, N_SEQ, slab_width), (1, 0, 2))
    down_slabs = down_mat.reshape(N_SEQ, slab_width, model_width)

    def add_slab(running, slab_pair):
        slab_out = jnp.dot(slab_pair[0], slab_pair[1], preferred_element_type=jnp.float32).astype(jnp.bfloat16)
        slab_out = lax.optimization_barrier(slab_out)
        return (running + slab_out.astype(jnp.float32), None)
    running, _ = lax.scan(add_slab, jnp.zeros((row_count, model_width), jnp.float32), (inner_slabs, down_slabs))
    return running.astype(jnp.bfloat16)

def reference(queries, key_rows, value_rows, decay_log, residual, out_gate, attn_gain, moe_gain, routes, route_weights, w_gate, w_up, w_down):
    sequence_length = queries.shape[0]
    blocks = sequence_length // BLOCK
    model_width = HEAD_COUNT * HEAD
    query_blocks = queries.reshape(blocks, BLOCK, HEAD_COUNT, HEAD)
    key_blocks = key_rows.reshape(blocks, BLOCK, HEAD_COUNT, HEAD)
    value_blocks = value_rows.reshape(blocks, BLOCK, HEAD_COUNT, HEAD)
    decay_blocks = decay_log.reshape(blocks, BLOCK, HEAD_COUNT)
    start_state = jnp.zeros((HEAD_COUNT, HEAD, HEAD), jnp.float32)
    final_state, mixed_out = lax.scan(block_attention, start_state, (query_blocks, key_blocks, value_blocks, decay_blocks))
    attended = mixed_out.reshape(sequence_length, model_width)
    attn_scale = lax.rsqrt(lax.optimization_barrier(jnp.mean(attended * attended, axis=1, keepdims=True)) + EPSILON)
    hidden = residual.astype(jnp.float32) + jax.nn.sigmoid(out_gate.astype(jnp.float32)) * (attended * attn_scale * attn_gain)
    second = lax.rsqrt(lax.optimization_barrier(jnp.mean(hidden * hidden, axis=1, keepdims=True)) + EPSILON)
    normed = (hidden * second * moe_gain).astype(jnp.bfloat16)
    experts = w_gate.shape[0]
    tables = jax.vmap(partial(slot_tables, experts=experts, capacity=CAP))
    dispatch, combine = tables(routes.reshape(N_SEQ, BLOCK, 2), route_weights.reshape(N_SEQ, BLOCK, 2))
    gathered = jnp.einsum('sbc,sbd->scd', dispatch, normed.reshape(N_SEQ, BLOCK, model_width).astype(jnp.float32)).astype(jnp.bfloat16)
    per_expert = jnp.transpose(gathered.reshape(N_SEQ, experts, CAP, model_width), (1, 0, 2, 3)).reshape(experts, N_SEQ * CAP, model_width)
    outputs = lax.map(expert_apply, (per_expert, w_gate, w_up, w_down))
    returned = jnp.transpose(outputs.reshape(experts, N_SEQ, CAP, model_width), (1, 0, 2, 3)).reshape(N_SEQ, experts * CAP, model_width)
    expert_mix = jnp.einsum('sbc,scd->sbd', combine, returned.astype(jnp.float32), precision=lax.Precision.HIGHEST)
    return (hidden + expert_mix.reshape(sequence_length, model_width)).astype(jnp.bfloat16)
```

```python
import jax
import jax.numpy as jnp
from jax import lax
from jax.sharding import PartitionSpec as P

CAP = 6


EPSILON = 1e-06

F32 = jnp.float32
BF16 = jnp.bfloat16


def three_terms(x):
    high = lax.reduce_precision(x, 8, 7)
    rest = x - high
    middle = lax.reduce_precision(rest, 8, 7)
    low = rest - middle
    return jnp.stack([high, middle, low]).astype(BF16)


def slot_tables(route_block, weight_block, experts, capacity):
    expert_ids = jnp.arange(experts, dtype=jnp.int32)
    onehot = (route_block[:, :, None] == expert_ids[None, None, :]).astype(jnp.int32)
    tokens = route_block.shape[0]
    flat_hits = onehot.reshape(tokens * 2, experts)
    before = jnp.cumsum(flat_hits, axis=0) - flat_hits
    places = jnp.arange(capacity, dtype=jnp.int32)
    hit_table = flat_hits[:, :, None] * (before[:, :, None] == places[None, None, :]).astype(
        jnp.int32
    )
    hit_table = hit_table.astype(jnp.float32).reshape(tokens, 2, experts * capacity)
    dispatch = jnp.sum(hit_table, axis=1)
    combine = jnp.sum(hit_table * weight_block[:, :, None], axis=1)
    return (dispatch, combine)


def padded_rows(x, rows):
    return jnp.pad(x, [(0, 0)] * (x.ndim - 2) + [(0, rows - x.shape[-2]), (0, 0)])


def project_rows(slot_rows, weight_rows):
    return lax.dot_general(
        slot_rows, weight_rows, (((1,), (1,)), ((), ())), preferred_element_type=jnp.float32
    )


def shards(
    queries,
    key_rows,
    value_rows,
    decay_log,
    residual,
    out_gate,
    attn_gain,
    moe_gain,
    routes,
    route_weights,
    w_gate,
    w_up,
    w_down,
):
    tokens, columns = queries.shape
    heads = decay_log.shape[1]
    lanes = columns // heads
    blocks = lax.axis_size("seq")
    near = heads
    far = blocks // near
    experts = lax.axis_size("exp")
    copies = lax.axis_size("rep")
    owners = experts * copies
    width = columns * owners
    half_cap = CAP // copies
    near_groups = [[near * i + k for k in range(near)] for i in range(far)]
    far_groups = [[i + near * k for k in range(far)] for i in range(near)]
    near_all = [[m * owners + j for m in group for j in range(owners)] for group in near_groups]
    my_far = lax.axis_index("seq") // near

    def by_head(x):
        return jnp.swapaxes(x.reshape(tokens, heads, lanes), 0, 1)

    cumulative = jnp.cumsum(decay_log, axis=0)
    terms = jnp.swapaxes(three_terms(cumulative), 0, 2)
    terms = jnp.swapaxes(terms, 1, 2)
    terms = jnp.pad(terms, ((0, 0), (0, 5), (0, lanes - tokens)))
    payload = jnp.concatenate(
        [by_head(queries), by_head(key_rows), by_head(value_rows), terms], axis=1
    )
    arrived = lax.all_to_all(payload, "seq", 0, 0, tiled=True, axis_index_groups=near_groups)
    span = near * tokens
    query = arrived[:, :tokens].reshape(span, lanes)
    key = arrived[:, tokens : 2 * tokens].reshape(span, lanes)
    value = arrived[:, 2 * tokens : 3 * tokens].reshape(span, lanes)
    within = arrived[:, 3 * tokens : 3 * tokens + 3, :tokens].astype(F32).sum(axis=1)
    ends = within[:, -1]
    starts = jnp.cumsum(ends) - ends
    total = jnp.sum(ends)
    cum = (within + starts[:, None]).reshape(span)
    faded = (key.astype(F32) * jnp.exp(total - cum)[:, None]).astype(BF16)
    state = lax.dot_general(faded, value, (((0,), (0,)), ((), ())), preferred_element_type=F32)
    total_rows = jnp.pad(jnp.broadcast_to(three_terms(total)[:, None], (3, lanes)), ((0, 5), (0, 0)))
    sent = jnp.concatenate([state.astype(BF16), total_rows], axis=0)
    states = lax.all_gather(sent, "seq", axis=0, tiled=False, axis_index_groups=far_groups)
    totals = states[:, lanes : lanes + 3, 0].astype(F32).sum(axis=1)
    reached = jnp.cumsum(totals)
    order = jnp.arange(far)
    before_mine = jnp.sum(jnp.where(order < my_far, totals, 0.0))
    earlier = order < my_far
    factors = jnp.where(earlier, jnp.exp(jnp.where(earlier, before_mine - reached, 0.0)), 0.0)
    incoming = jnp.sum(factors[:, None, None] * states[:, :lanes].astype(F32), axis=0)
    scores = lax.dot_general(query, key, (((1,), (1,)), ((), ())), preferred_element_type=F32)
    places = jnp.arange(span)
    causal = places[:, None] >= places[None, :]
    decays = jnp.where(causal, jnp.exp(jnp.where(causal, cum[:, None] - cum[None, :], 0.0)), 0.0)
    mixing = (scores * decays).astype(BF16)
    lifted = (query.astype(F32) * jnp.exp(cum)[:, None]).astype(BF16)
    attended = jnp.dot(mixing, value, preferred_element_type=F32) + jnp.dot(
        lifted, incoming.astype(BF16), preferred_element_type=F32
    )
    attended = attended.astype(BF16).reshape(near, tokens, lanes)
    attended = lax.all_to_all(attended, "seq", 0, 0, tiled=True, axis_index_groups=near_groups)
    attended = jnp.swapaxes(attended, 0, 1).reshape(tokens, columns).astype(F32)

    sumsq = jnp.sum(attended * attended, axis=1)
    branch = jax.nn.sigmoid(out_gate.astype(F32)) * attended * attn_gain
    dispatch, combine = slot_tables(routes, route_weights, experts, CAP)
    both = jnp.concatenate([residual, branch.astype(BF16)], axis=1)
    packed = jnp.dot(jnp.transpose(dispatch).astype(BF16), both, preferred_element_type=F32)
    packed = packed.astype(BF16).reshape(owners, half_cap * 2 * heads, lanes)
    sums = jnp.pad(three_terms(sumsq), ((0, 0), (0, lanes - tokens)))
    gains = three_terms(moe_gain).reshape(3 * heads, lanes)
    extra = jnp.concatenate([sums, gains], axis=0)
    extra = padded_rows(extra, 16)
    extra = jnp.broadcast_to(extra[None], (owners, *extra.shape))
    payload = jnp.concatenate([packed, extra], axis=1)
    arrived = lax.all_to_all(payload, ("exp", "rep"), 0, 0, tiled=True)
    size = half_cap * 2 * heads
    rows = arrived[:, :size].reshape(owners, half_cap, 2, columns).astype(F32)
    sums = arrived[:, size : size + 3, :tokens].astype(F32).sum(axis=(0, 1))
    gains = arrived[:, size + 3 : size + 3 + 3 * heads].astype(F32)
    gains = gains.reshape(owners, 3, columns).sum(axis=1)
    attn_scale = lax.rsqrt(sums / width + EPSILON)
    me = lax.axis_index(("exp", "rep"))
    mine = lax.dynamic_slice_in_dim(dispatch, me * half_cap, half_cap, axis=1)
    slot_scale = jnp.sum(mine * attn_scale[:, None], axis=0)
    slot_hidden = rows[:, :, 0] + slot_scale[None, :, None] * rows[:, :, 1]
    moe_sumsq = jnp.sum(slot_hidden * slot_hidden, axis=(0, 2))
    moe_scale = lax.rsqrt(moe_sumsq / width + EPSILON)
    normed = (slot_hidden * moe_scale[None, :, None] * gains[:, None, :]).astype(BF16)
    normed = jnp.swapaxes(normed, 0, 1).reshape(half_cap * width // lanes, lanes)

    gathered = lax.all_gather(normed, "seq", axis=0, tiled=True, axis_index_groups=far_groups)
    gathered = lax.all_gather(gathered, "seq", axis=0, tiled=True, axis_index_groups=near_groups)
    slot_rows = gathered.reshape(blocks * half_cap, width)
    gate_val = project_rows(slot_rows, w_gate[0])
    up_val = project_rows(slot_rows, w_up[0])
    inner = (jax.nn.silu(gate_val) * up_val).astype(BF16)
    partial = jnp.dot(inner, w_down[0], preferred_element_type=F32).astype(BF16)
    pieces = partial.reshape(near, far * half_cap, owners, columns)
    pieces = jnp.swapaxes(pieces, 1, 2).reshape(near * owners, far * half_cap, columns)
    pieces = lax.all_to_all(
        pieces, ("seq", "exp", "rep"), 0, 0, tiled=True, axis_index_groups=near_all
    )
    pieces = pieces.reshape(near, owners, far, half_cap, columns).astype(F32).sum(axis=0)
    pieces = jnp.swapaxes(pieces.astype(BF16), 0, 1).reshape(far, owners * half_cap, columns)
    pieces = lax.all_to_all(pieces, "seq", 0, 0, tiled=True, axis_index_groups=far_groups)
    returned = pieces.astype(F32).sum(axis=0).astype(BF16)
    expert_mix = jnp.dot(combine, returned.astype(F32), precision=lax.Precision.HIGHEST)
    hidden = residual.astype(F32) + attn_scale[:, None] * branch
    return (hidden + expert_mix).astype(BF16)


def solution(mesh):
    return jax.shard_map(
        shards,
        mesh=mesh,
        in_specs=(
            P(("groups", "seq"), ("exp", "rep")),
            P(("groups", "seq"), ("exp", "rep")),
            P(("groups", "seq"), ("exp", "rep")),
            P(("groups", "seq"), ("exp", "rep")),
            P(("groups", "seq"), ("exp", "rep")),
            P(("groups", "seq"), ("exp", "rep")),
            P(("exp", "rep")),
            P(("exp", "rep")),
            P(("groups", "seq"), None),
            P(("groups", "seq"), None),
            P("exp", "seq", None),
            P("exp", "seq", None),
            P("exp", "seq", None),
        ),
        out_specs=P(("groups", "seq"), ("exp", "rep")),
        check_vma=False,
    )
```

```python
import jax
import jax.numpy as jnp
from jax import lax
from jax.sharding import PartitionSpec as P

CAP = 6


EPSILON = 1e-06

F32 = jnp.float32
BF16 = jnp.bfloat16


def three_terms(x):
    high = lax.reduce_precision(x, 8, 7)
    rest = x - high
    middle = lax.reduce_precision(rest, 8, 7)
    low = rest - middle
    return jnp.stack([high, middle, low]).astype(BF16)


def slot_tables(route_block, weight_block, experts, capacity):
    expert_ids = jnp.arange(experts, dtype=jnp.int32)
    onehot = (route_block[:, :, None] == expert_ids[None, None, :]).astype(jnp.int32)
    tokens = route_block.shape[0]
    flat_hits = onehot.reshape(tokens * 2, experts)
    before = jnp.cumsum(flat_hits, axis=0) - flat_hits
    places = jnp.arange(capacity, dtype=jnp.int32)
    hit_table = flat_hits[:, :, None] * (before[:, :, None] == places[None, None, :]).astype(
        jnp.int32
    )
    hit_table = hit_table.astype(jnp.float32).reshape(tokens, 2, experts * capacity)
    dispatch = jnp.sum(hit_table, axis=1)
    combine = jnp.sum(hit_table * weight_block[:, :, None], axis=1)
    return (dispatch, combine)


def padded_rows(x, rows):
    return jnp.pad(x, [(0, 0)] * (x.ndim - 2) + [(0, rows - x.shape[-2]), (0, 0)])


def project_rows(slot_rows, weight_rows):
    return lax.dot_general(
        slot_rows, weight_rows, (((1,), (1,)), ((), ())), preferred_element_type=jnp.float32
    )


def shards(
    queries,
    key_rows,
    value_rows,
    decay_log,
    residual,
    out_gate,
    attn_gain,
    moe_gain,
    routes,
    route_weights,
    w_gate,
    w_up,
    w_down,
):
    tokens, columns = queries.shape
    heads = decay_log.shape[1]
    lanes = columns // heads
    blocks = lax.axis_size("seq")
    near = heads
    far = blocks // near
    experts = lax.axis_size("exp")
    copies = lax.axis_size("rep")
    owners = experts * copies
    width = columns * owners
    half_cap = CAP // copies
    near_groups = [[near * i + k for k in range(near)] for i in range(far)]
    far_groups = [[i + near * k for k in range(far)] for i in range(near)]
    near_all = [[m * owners + j for m in group for j in range(owners)] for group in near_groups]

    def by_head(x):
        return jnp.swapaxes(x.reshape(tokens, heads, lanes), 0, 1)

    cumulative = jnp.cumsum(decay_log, axis=0)
    terms = jnp.swapaxes(three_terms(cumulative), 0, 2)
    terms = jnp.swapaxes(terms, 1, 2)
    terms = jnp.pad(terms, ((0, 0), (0, 5), (0, lanes - tokens)))
    payload = jnp.concatenate(
        [by_head(queries), by_head(key_rows), by_head(value_rows), terms], axis=1
    )
    arrived = lax.all_to_all(payload, "seq", 0, 0, tiled=True, axis_index_groups=near_groups)
    span = near * tokens
    query = arrived[:, :tokens].reshape(span, lanes)
    key = arrived[:, tokens : 2 * tokens].reshape(span, lanes)
    value = arrived[:, 2 * tokens : 3 * tokens].reshape(span, lanes)
    within = arrived[:, 3 * tokens : 3 * tokens + 3, :tokens].astype(F32).sum(axis=1)
    ends = within[:, -1]
    starts = jnp.cumsum(ends) - ends
    total = jnp.sum(ends)
    cum = (within + starts[:, None]).reshape(span)
    faded = (key.astype(F32) * jnp.exp(total - cum)[:, None]).astype(BF16)
    state = lax.dot_general(faded, value, (((0,), (0,)), ((), ())), preferred_element_type=F32)
    carried = jnp.zeros_like(state)
    for k in range(far - 1):
        running = (jnp.exp(total) * carried + state).astype(BF16)
        passed = [(near * k + i, near * (k + 1) + i) for i in range(near)]
        carried = carried + lax.ppermute(running, "seq", passed).astype(F32)
    incoming = carried
    scores = lax.dot_general(query, key, (((1,), (1,)), ((), ())), preferred_element_type=F32)
    places = jnp.arange(span)
    causal = places[:, None] >= places[None, :]
    decays = jnp.where(causal, jnp.exp(jnp.where(causal, cum[:, None] - cum[None, :], 0.0)), 0.0)
    mixing = (scores * decays).astype(BF16)
    lifted = (query.astype(F32) * jnp.exp(cum)[:, None]).astype(BF16)
    attended = jnp.dot(mixing, value, preferred_element_type=F32) + jnp.dot(
        lifted, incoming.astype(BF16), preferred_element_type=F32
    )
    attended = attended.astype(BF16).reshape(near, tokens, lanes)
    attended = lax.all_to_all(attended, "seq", 0, 0, tiled=True, axis_index_groups=near_groups)
    attended = jnp.swapaxes(attended, 0, 1).reshape(tokens, columns).astype(F32)

    sumsq = jnp.sum(attended * attended, axis=1)
    branch = jax.nn.sigmoid(out_gate.astype(F32)) * attended * attn_gain
    dispatch, combine = slot_tables(routes, route_weights, experts, CAP)
    both = jnp.concatenate([residual, branch.astype(BF16)], axis=1)
    packed = jnp.dot(jnp.transpose(dispatch).astype(BF16), both, preferred_element_type=F32)
    packed = packed.astype(BF16).reshape(owners, half_cap * 2 * heads, lanes)
    sums = jnp.pad(three_terms(sumsq), ((0, 0), (0, lanes - tokens)))
    gains = three_terms(moe_gain).reshape(3 * heads, lanes)
    extra = jnp.concatenate([sums, gains], axis=0)
    extra = padded_rows(extra, 16)
    extra = jnp.broadcast_to(extra[None], (owners, *extra.shape))
    payload = jnp.concatenate([packed, extra], axis=1)
    arrived = lax.all_to_all(payload, ("exp", "rep"), 0, 0, tiled=True)
    size = half_cap * 2 * heads
    rows = arrived[:, :size].reshape(owners, half_cap, 2, columns).astype(F32)
    sums = arrived[:, size : size + 3, :tokens].astype(F32).sum(axis=(0, 1))
    gains = arrived[:, size + 3 : size + 3 + 3 * heads].astype(F32)
    gains = gains.reshape(owners, 3, columns).sum(axis=1)
    attn_scale = lax.rsqrt(sums / width + EPSILON)
    me = lax.axis_index(("exp", "rep"))
    mine = lax.dynamic_slice_in_dim(dispatch, me * half_cap, half_cap, axis=1)
    slot_scale = jnp.sum(mine * attn_scale[:, None], axis=0)
    slot_hidden = rows[:, :, 0] + slot_scale[None, :, None] * rows[:, :, 1]
    moe_sumsq = jnp.sum(slot_hidden * slot_hidden, axis=(0, 2))
    moe_scale = lax.rsqrt(moe_sumsq / width + EPSILON)
    normed = (slot_hidden * moe_scale[None, :, None] * gains[:, None, :]).astype(BF16)
    normed = jnp.swapaxes(normed, 0, 1).reshape(half_cap * width // lanes, lanes)

    gathered = lax.all_gather(normed, "seq", axis=0, tiled=True, axis_index_groups=far_groups)
    gathered = lax.all_gather(gathered, "seq", axis=0, tiled=True, axis_index_groups=near_groups)
    slot_rows = gathered.reshape(blocks * half_cap, width)
    gate_val = project_rows(slot_rows, w_gate[0])
    up_val = project_rows(slot_rows, w_up[0])
    inner = (jax.nn.silu(gate_val) * up_val).astype(BF16)
    partial = jnp.dot(inner, w_down[0], preferred_element_type=F32).astype(BF16)
    pieces = partial.reshape(near, far * half_cap, owners, columns)
    pieces = jnp.swapaxes(pieces, 1, 2).reshape(near * owners, far * half_cap, columns)
    pieces = lax.all_to_all(
        pieces, ("seq", "exp", "rep"), 0, 0, tiled=True, axis_index_groups=near_all
    )
    pieces = pieces.reshape(near, owners, far, half_cap, columns).astype(F32).sum(axis=0)
    pieces = jnp.swapaxes(pieces.astype(BF16), 0, 1).reshape(far, owners * half_cap, columns)
    pieces = lax.all_to_all(pieces, "seq", 0, 0, tiled=True, axis_index_groups=far_groups)
    returned = pieces.astype(F32).sum(axis=0).astype(BF16)
    expert_mix = jnp.dot(combine, returned.astype(F32), precision=lax.Precision.HIGHEST)
    hidden = residual.astype(F32) + attn_scale[:, None] * branch
    return (hidden + expert_mix).astype(BF16)


def solution(mesh):
    return jax.shard_map(
        shards,
        mesh=mesh,
        in_specs=(
            P(("groups", "seq"), ("exp", "rep")),
            P(("groups", "seq"), ("exp", "rep")),
            P(("groups", "seq"), ("exp", "rep")),
            P(("groups", "seq"), ("exp", "rep")),
            P(("groups", "seq"), ("exp", "rep")),
            P(("groups", "seq"), ("exp", "rep")),
            P(("exp", "rep")),
            P(("exp", "rep")),
            P(("groups", "seq"), None),
            P(("groups", "seq"), None),
            P("exp", "seq", None),
            P("exp", "seq", None),
            P("exp", "seq", None),
        ),
        out_specs=P(("groups", "seq"), ("exp", "rep")),
        check_vma=False,
    )
```

```python
import jax
import jax.numpy as jnp
from jax import lax
from jax.sharding import PartitionSpec as P

CAP = 6


EPSILON = 1e-06

F32 = jnp.float32
BF16 = jnp.bfloat16


def three_terms(x):
    high = lax.reduce_precision(x, 8, 7)
    rest = x - high
    middle = lax.reduce_precision(rest, 8, 7)
    low = rest - middle
    return jnp.stack([high, middle, low]).astype(BF16)


def slot_tables(route_block, weight_block, experts, capacity):
    expert_ids = jnp.arange(experts, dtype=jnp.int32)
    onehot = (route_block[:, :, None] == expert_ids[None, None, :]).astype(jnp.int32)
    tokens = route_block.shape[0]
    flat_hits = onehot.reshape(tokens * 2, experts)
    before = jnp.cumsum(flat_hits, axis=0) - flat_hits
    places = jnp.arange(capacity, dtype=jnp.int32)
    hit_table = flat_hits[:, :, None] * (before[:, :, None] == places[None, None, :]).astype(
        jnp.int32
    )
    hit_table = hit_table.astype(jnp.float32).reshape(tokens, 2, experts * capacity)
    dispatch = jnp.sum(hit_table, axis=1)
    combine = jnp.sum(hit_table * weight_block[:, :, None], axis=1)
    return (dispatch, combine)


def padded_rows(x, rows):
    return jnp.pad(x, [(0, 0)] * (x.ndim - 2) + [(0, rows - x.shape[-2]), (0, 0)])


def project_rows(slot_rows, weight_rows):
    return lax.dot_general(
        slot_rows, weight_rows, (((1,), (1,)), ((), ())), preferred_element_type=jnp.float32
    )


def shards(
    queries,
    key_rows,
    value_rows,
    decay_log,
    residual,
    out_gate,
    attn_gain,
    moe_gain,
    routes,
    route_weights,
    w_gate,
    w_up,
    w_down,
):
    tokens, columns = queries.shape
    heads = decay_log.shape[1]
    lanes = columns // heads
    blocks = lax.axis_size("seq")
    near = heads
    far = blocks // near
    experts = lax.axis_size("exp")
    copies = lax.axis_size("rep")
    owners = experts * copies
    width = columns * owners
    half_cap = CAP // copies
    near_groups = [[near * i + k for k in range(near)] for i in range(far)]
    far_groups = [[i + near * k for k in range(far)] for i in range(near)]
    near_all = [[m * owners + j for m in group for j in range(owners)] for group in near_groups]

    def by_head(x):
        return jnp.swapaxes(x.reshape(tokens, heads, lanes), 0, 1)

    cumulative = jnp.cumsum(decay_log, axis=0)
    terms = jnp.swapaxes(three_terms(cumulative), 0, 2)
    terms = jnp.swapaxes(terms, 1, 2)
    terms = jnp.pad(terms, ((0, 0), (0, 5), (0, lanes - tokens)))
    payload = jnp.concatenate(
        [by_head(queries), by_head(key_rows), by_head(value_rows), terms], axis=1
    )
    arrived = lax.all_to_all(payload, "seq", 0, 0, tiled=True, axis_index_groups=near_groups)
    span = near * tokens
    query = arrived[:, :tokens].reshape(span, lanes)
    key = arrived[:, tokens : 2 * tokens].reshape(span, lanes)
    value = arrived[:, 2 * tokens : 3 * tokens].reshape(span, lanes)
    within = arrived[:, 3 * tokens : 3 * tokens + 3, :tokens].astype(F32).sum(axis=1)
    ends = within[:, -1]
    starts = jnp.cumsum(ends) - ends
    total = jnp.sum(ends)
    cum = (within + starts[:, None]).reshape(span)
    faded = (key.astype(F32) * jnp.exp(total - cum)[:, None]).astype(BF16)
    state = lax.dot_general(faded, value, (((0,), (0,)), ((), ())), preferred_element_type=F32)
    my_far = lax.axis_index("seq") // near
    fade = jnp.exp(total)
    carried = jnp.zeros((lanes + 8, lanes), F32)
    for k in range(1, far - 1):
        factor = jnp.where(my_far >= 2, carried[lanes] + carried[lanes + 1], 1.0) * fade
        high = lax.reduce_precision(factor, 8, 7)
        tail = jnp.pad(jnp.stack([high, factor - high]), ((0, 6), (0, 0)))
        running = jnp.concatenate([fade * carried[:lanes] + state, tail], axis=0).astype(BF16)
        passed = [(near * k + i, near * (k + 1) + i) for i in range(near)]
        carried = carried + lax.ppermute(running, "seq", passed).astype(F32)
    factor = jnp.where(my_far >= 2, carried[lanes] + carried[lanes + 1], 1.0)
    first = jnp.where(my_far == 0, state.astype(BF16), running[:lanes])
    order = sorted(range(1, far), key=lambda g: (g != 1, min(g, far - g), g))
    from_first = [
        lax.ppermute(first, "seq", [(i, near * g + i) for i in range(near)]) for g in order
    ]
    from_first = sum(x.astype(F32) for x in from_first)
    incoming = carried[:lanes] + factor[0] * from_first
    scores = lax.dot_general(query, key, (((1,), (1,)), ((), ())), preferred_element_type=F32)
    places = jnp.arange(span)
    causal = places[:, None] >= places[None, :]
    decays = jnp.where(causal, jnp.exp(jnp.where(causal, cum[:, None] - cum[None, :], 0.0)), 0.0)
    mixing = (scores * decays).astype(BF16)
    lifted = (query.astype(F32) * jnp.exp(cum)[:, None]).astype(BF16)
    attended = jnp.dot(mixing, value, preferred_element_type=F32) + jnp.dot(
        lifted, incoming.astype(BF16), preferred_element_type=F32
    )
    attended = attended.astype(BF16).reshape(near, tokens, lanes)
    attended = lax.all_to_all(attended, "seq", 0, 0, tiled=True, axis_index_groups=near_groups)
    attended = jnp.swapaxes(attended, 0, 1).reshape(tokens, columns).astype(F32)

    sumsq = jnp.sum(attended * attended, axis=1)
    branch = jax.nn.sigmoid(out_gate.astype(F32)) * attended * attn_gain
    dispatch, combine = slot_tables(routes, route_weights, experts, CAP)
    both = jnp.concatenate([residual, branch.astype(BF16)], axis=1)
    packed = jnp.dot(jnp.transpose(dispatch).astype(BF16), both, preferred_element_type=F32)
    packed = packed.astype(BF16).reshape(owners, half_cap * 2 * heads, lanes)
    sums = jnp.pad(three_terms(sumsq), ((0, 0), (0, lanes - tokens)))
    gains = three_terms(moe_gain).reshape(3 * heads, lanes)
    extra = jnp.concatenate([sums, gains], axis=0)
    extra = padded_rows(extra, 16)
    extra = jnp.broadcast_to(extra[None], (owners, *extra.shape))
    payload = jnp.concatenate([packed, extra], axis=1)
    arrived = lax.all_to_all(payload, ("exp", "rep"), 0, 0, tiled=True)
    size = half_cap * 2 * heads
    rows = arrived[:, :size].reshape(owners, half_cap, 2, columns).astype(F32)
    sums = arrived[:, size : size + 3, :tokens].astype(F32).sum(axis=(0, 1))
    gains = arrived[:, size + 3 : size + 3 + 3 * heads].astype(F32)
    gains = gains.reshape(owners, 3, columns).sum(axis=1)
    attn_scale = lax.rsqrt(sums / width + EPSILON)
    me = lax.axis_index(("exp", "rep"))
    mine = lax.dynamic_slice_in_dim(dispatch, me * half_cap, half_cap, axis=1)
    slot_scale = jnp.sum(mine * attn_scale[:, None], axis=0)
    slot_hidden = rows[:, :, 0] + slot_scale[None, :, None] * rows[:, :, 1]
    moe_sumsq = jnp.sum(slot_hidden * slot_hidden, axis=(0, 2))
    moe_scale = lax.rsqrt(moe_sumsq / width + EPSILON)
    normed = (slot_hidden * moe_scale[None, :, None] * gains[:, None, :]).astype(BF16)
    normed = jnp.swapaxes(normed, 0, 1).reshape(half_cap * width // lanes, lanes)

    gathered = lax.all_gather(normed, "seq", axis=0, tiled=True, axis_index_groups=far_groups)
    gathered = lax.all_gather(gathered, "seq", axis=0, tiled=True, axis_index_groups=near_groups)
    slot_rows = gathered.reshape(blocks * half_cap, width)
    gate_val = project_rows(slot_rows, w_gate[0])
    up_val = project_rows(slot_rows, w_up[0])
    inner = (jax.nn.silu(gate_val) * up_val).astype(BF16)
    partial = jnp.dot(inner, w_down[0], preferred_element_type=F32).astype(BF16)
    pieces = partial.reshape(near, far * half_cap, owners, columns)
    pieces = jnp.swapaxes(pieces, 1, 2).reshape(near * owners, far * half_cap, columns)
    pieces = lax.all_to_all(
        pieces, ("seq", "exp", "rep"), 0, 0, tiled=True, axis_index_groups=near_all
    )
    pieces = pieces.reshape(near, owners, far, half_cap, columns).astype(F32).sum(axis=0)
    pieces = jnp.swapaxes(pieces.astype(BF16), 0, 1).reshape(far, owners * half_cap, columns)
    pieces = lax.all_to_all(pieces, "seq", 0, 0, tiled=True, axis_index_groups=far_groups)
    returned = pieces.astype(F32).sum(axis=0).astype(BF16)
    expert_mix = jnp.dot(combine, returned.astype(F32), precision=lax.Precision.HIGHEST)
    hidden = residual.astype(F32) + attn_scale[:, None] * branch
    return (hidden + expert_mix).astype(BF16)


def solution(mesh):
    return jax.shard_map(
        shards,
        mesh=mesh,
        in_specs=(
            P(("groups", "seq"), ("exp", "rep")),
            P(("groups", "seq"), ("exp", "rep")),
            P(("groups", "seq"), ("exp", "rep")),
            P(("groups", "seq"), ("exp", "rep")),
            P(("groups", "seq"), ("exp", "rep")),
            P(("groups", "seq"), ("exp", "rep")),
            P(("exp", "rep")),
            P(("exp", "rep")),
            P(("groups", "seq"), None),
            P(("groups", "seq"), None),
            P("exp", "seq", None),
            P("exp", "seq", None),
            P("exp", "seq", None),
        ),
        out_specs=P(("groups", "seq"), ("exp", "rep")),
        check_vma=False,
    )
```

```python
import jax
import jax.numpy as jnp
from jax import lax
from jax.sharding import PartitionSpec as P

CAP = 6


EPSILON = 1e-06

F32 = jnp.float32
BF16 = jnp.bfloat16


def three_terms(x):
    high = lax.reduce_precision(x, 8, 7)
    rest = x - high
    middle = lax.reduce_precision(rest, 8, 7)
    low = rest - middle
    return jnp.stack([high, middle, low]).astype(BF16)


def slot_tables(route_block, weight_block, experts, capacity):
    expert_ids = jnp.arange(experts, dtype=jnp.int32)
    onehot = (route_block[:, :, None] == expert_ids[None, None, :]).astype(jnp.int32)
    tokens = route_block.shape[0]
    flat_hits = onehot.reshape(tokens * 2, experts)
    before = jnp.cumsum(flat_hits, axis=0) - flat_hits
    places = jnp.arange(capacity, dtype=jnp.int32)
    hit_table = flat_hits[:, :, None] * (before[:, :, None] == places[None, None, :]).astype(
        jnp.int32
    )
    hit_table = hit_table.astype(jnp.float32).reshape(tokens, 2, experts * capacity)
    dispatch = jnp.sum(hit_table, axis=1)
    combine = jnp.sum(hit_table * weight_block[:, :, None], axis=1)
    return (dispatch, combine)


def padded_rows(x, rows):
    return jnp.pad(x, [(0, 0)] * (x.ndim - 2) + [(0, rows - x.shape[-2]), (0, 0)])


def project_rows(slot_rows, weight_rows):
    return lax.dot_general(
        slot_rows, weight_rows, (((1,), (1,)), ((), ())), preferred_element_type=jnp.float32
    )


def shards(
    queries,
    key_rows,
    value_rows,
    decay_log,
    residual,
    out_gate,
    attn_gain,
    moe_gain,
    routes,
    route_weights,
    w_gate,
    w_up,
    w_down,
):
    tokens, columns = queries.shape
    heads = decay_log.shape[1]
    lanes = columns // heads
    blocks = lax.axis_size("seq")
    near = heads
    far = blocks // near
    experts = lax.axis_size("exp")
    copies = lax.axis_size("rep")
    owners = experts * copies
    width = columns * owners
    half_cap = CAP // copies
    near_groups = [[near * i + k for k in range(near)] for i in range(far)]
    far_groups = [[i + near * k for k in range(far)] for i in range(near)]
    near_all = [[m * owners + j for m in group for j in range(owners)] for group in near_groups]

    def by_head(x):
        return jnp.swapaxes(x.reshape(tokens, heads, lanes), 0, 1)

    cumulative = jnp.cumsum(decay_log, axis=0)
    terms = jnp.swapaxes(three_terms(cumulative), 0, 2)
    terms = jnp.swapaxes(terms, 1, 2)
    terms = jnp.pad(terms, ((0, 0), (0, 5), (0, lanes - tokens)))
    payload = jnp.concatenate(
        [by_head(queries), by_head(key_rows), by_head(value_rows), terms], axis=1
    )
    arrived = lax.all_to_all(payload, "seq", 0, 0, tiled=True, axis_index_groups=near_groups)
    span = near * tokens
    query = arrived[:, :tokens].reshape(span, lanes)
    key = arrived[:, tokens : 2 * tokens].reshape(span, lanes)
    value = arrived[:, 2 * tokens : 3 * tokens].reshape(span, lanes)
    within = arrived[:, 3 * tokens : 3 * tokens + 3, :tokens].astype(F32).sum(axis=1)
    ends = within[:, -1]
    starts = jnp.cumsum(ends) - ends
    total = jnp.sum(ends)
    cum = (within + starts[:, None]).reshape(span)
    faded = (key.astype(F32) * jnp.exp(total - cum)[:, None]).astype(BF16)
    state = lax.dot_general(faded, value, (((0,), (0,)), ((), ())), preferred_element_type=F32)
    my_far = lax.axis_index("seq") // near
    fade = jnp.exp(total)
    first = state.astype(BF16)
    order = sorted(range(1, far), key=lambda g: (g != 1, min(g, far - g), -g))
    from_first = []
    for g in order:
        from_first.append(
            lax.ppermute(first, "seq", [(i, near * g + i) for i in range(near)])
        )
    scales = jnp.exp2(jnp.arange(8, dtype=F32) / 8)[:, None]
    scales = jnp.broadcast_to(scales, (8, lanes))
    own = jnp.pad(state, ((0, 8), (0, 0)))
    opening = jnp.where(my_far <= 1, scales, 0.0)
    carried = jnp.pad(opening, ((lanes, 0), (0, 0)))
    for k in range(1, far - 1):
        running = (fade * carried + own).astype(BF16)
        passed = [(near * k + i, near * (k + 1) + i) for i in range(near)]
        received = lax.ppermute(running, "seq", passed)
        carried = carried + received.astype(F32)
    factor = jnp.mean(carried[lanes:] / scales, axis=0)
    from_first = sum(x.astype(F32) for x in from_first)
    incoming = carried[:lanes] + factor * from_first
    scores = lax.dot_general(query, key, (((1,), (1,)), ((), ())), preferred_element_type=F32)
    places = jnp.arange(span)
    causal = places[:, None] >= places[None, :]
    decays = jnp.where(causal, jnp.exp(jnp.where(causal, cum[:, None] - cum[None, :], 0.0)), 0.0)
    mixing = (scores * decays).astype(BF16)
    lifted = (query.astype(F32) * jnp.exp(cum)[:, None]).astype(BF16)
    attended = jnp.dot(mixing, value, preferred_element_type=F32) + jnp.dot(
        lifted, incoming.astype(BF16), preferred_element_type=F32
    )
    attended = attended.astype(BF16).reshape(near, tokens, lanes)
    attended = lax.all_to_all(attended, "seq", 0, 0, tiled=True, axis_index_groups=near_groups)
    attended = jnp.swapaxes(attended, 0, 1).reshape(tokens, columns).astype(F32)

    sumsq = jnp.sum(attended * attended, axis=1)
    branch = jax.nn.sigmoid(out_gate.astype(F32)) * attended * attn_gain
    dispatch, combine = slot_tables(routes, route_weights, experts, CAP)
    both = jnp.concatenate([residual, branch.astype(BF16)], axis=1)
    packed = jnp.dot(jnp.transpose(dispatch).astype(BF16), both, preferred_element_type=F32)
    packed = packed.astype(BF16).reshape(owners, half_cap * 2 * heads, lanes)
    sums = jnp.pad(three_terms(sumsq), ((0, 0), (0, lanes - tokens)))
    gains = three_terms(moe_gain).reshape(3 * heads, lanes)
    extra = jnp.concatenate([sums, gains], axis=0)
    extra = padded_rows(extra, 16)
    extra = jnp.broadcast_to(extra[None], (owners, *extra.shape))
    payload = jnp.concatenate([packed, extra], axis=1)
    arrived = lax.all_to_all(payload, ("exp", "rep"), 0, 0, tiled=True)
    size = half_cap * 2 * heads
    rows = arrived[:, :size].reshape(owners, half_cap, 2, columns).astype(F32)
    sums = arrived[:, size : size + 3, :tokens].astype(F32).sum(axis=(0, 1))
    gains = arrived[:, size + 3 : size + 3 + 3 * heads].astype(F32)
    gains = gains.reshape(owners, 3, columns).sum(axis=1)
    attn_scale = lax.rsqrt(sums / width + EPSILON)
    me = lax.axis_index(("exp", "rep"))
    mine = lax.dynamic_slice_in_dim(dispatch, me * half_cap, half_cap, axis=1)
    slot_scale = jnp.sum(mine * attn_scale[:, None], axis=0)
    slot_hidden = rows[:, :, 0] + slot_scale[None, :, None] * rows[:, :, 1]
    moe_sumsq = jnp.sum(slot_hidden * slot_hidden, axis=(0, 2))
    moe_scale = lax.rsqrt(moe_sumsq / width + EPSILON)
    normed = (slot_hidden * moe_scale[None, :, None] * gains[:, None, :]).astype(BF16)
    normed = jnp.swapaxes(normed, 0, 1).reshape(half_cap * width // lanes, lanes)

    gathered = lax.all_gather(normed, "seq", axis=0, tiled=True, axis_index_groups=far_groups)
    gathered = lax.all_gather(gathered, "seq", axis=0, tiled=True, axis_index_groups=near_groups)
    slot_rows = gathered.reshape(blocks * half_cap, width)
    gate_val = project_rows(slot_rows, w_gate[0])
    up_val = project_rows(slot_rows, w_up[0])
    inner = (jax.nn.silu(gate_val) * up_val).astype(BF16)
    partial = jnp.dot(inner, w_down[0], preferred_element_type=F32).astype(BF16)
    pieces = partial.reshape(near, far * half_cap, owners, columns)
    pieces = jnp.swapaxes(pieces, 1, 2).reshape(near * owners, far * half_cap, columns)
    pieces = lax.all_to_all(
        pieces, ("seq", "exp", "rep"), 0, 0, tiled=True, axis_index_groups=near_all
    )
    pieces = pieces.reshape(near, owners, far, half_cap, columns).astype(F32).sum(axis=0)
    pieces = jnp.swapaxes(pieces.astype(BF16), 0, 1).reshape(far, owners * half_cap, columns)
    pieces = lax.all_to_all(pieces, "seq", 0, 0, tiled=True, axis_index_groups=far_groups)
    returned = pieces.astype(F32).sum(axis=0).astype(BF16)
    expert_mix = jnp.dot(combine, returned.astype(F32), precision=lax.Precision.HIGHEST)
    hidden = residual.astype(F32) + attn_scale[:, None] * branch
    return (hidden + expert_mix).astype(BF16)


def solution(mesh):
    return jax.shard_map(
        shards,
        mesh=mesh,
        in_specs=(
            P(("groups", "seq"), ("exp", "rep")),
            P(("groups", "seq"), ("exp", "rep")),
            P(("groups", "seq"), ("exp", "rep")),
            P(("groups", "seq"), ("exp", "rep")),
            P(("groups", "seq"), ("exp", "rep")),
            P(("groups", "seq"), ("exp", "rep")),
            P(("exp", "rep")),
            P(("exp", "rep")),
            P(("groups", "seq"), None),
            P(("groups", "seq"), None),
            P("exp", "seq", None),
            P("exp", "seq", None),
            P("exp", "seq", None),
        ),
        out_specs=P(("groups", "seq"), ("exp", "rep")),
        check_vma=False,
    )
```

```python
import jax
import jax.numpy as jnp
from jax import lax
from jax.sharding import PartitionSpec as P

CAP = 6


EPSILON = 1e-06

F32 = jnp.float32
BF16 = jnp.bfloat16


def three_terms(x):
    high = lax.reduce_precision(x, 8, 7)
    rest = x - high
    middle = lax.reduce_precision(rest, 8, 7)
    low = rest - middle
    return jnp.stack([high, middle, low]).astype(BF16)


def slot_tables(route_block, weight_block, experts, capacity):
    expert_ids = jnp.arange(experts, dtype=jnp.int32)
    onehot = (route_block[:, :, None] == expert_ids[None, None, :]).astype(jnp.int32)
    tokens = route_block.shape[0]
    flat_hits = onehot.reshape(tokens * 2, experts)
    before = jnp.cumsum(flat_hits, axis=0) - flat_hits
    places = jnp.arange(capacity, dtype=jnp.int32)
    hit_table = flat_hits[:, :, None] * (before[:, :, None] == places[None, None, :]).astype(
        jnp.int32
    )
    hit_table = hit_table.astype(jnp.float32).reshape(tokens, 2, experts * capacity)
    dispatch = jnp.sum(hit_table, axis=1)
    combine = jnp.sum(hit_table * weight_block[:, :, None], axis=1)
    return (dispatch, combine)


def padded_rows(x, rows):
    return jnp.pad(x, [(0, 0)] * (x.ndim - 2) + [(0, rows - x.shape[-2]), (0, 0)])


def project_rows(slot_rows, weight_rows):
    return lax.dot_general(
        slot_rows, weight_rows, (((1,), (1,)), ((), ())), preferred_element_type=jnp.float32
    )


def shards(
    queries,
    key_rows,
    value_rows,
    decay_log,
    residual,
    out_gate,
    attn_gain,
    moe_gain,
    routes,
    route_weights,
    w_gate,
    w_up,
    w_down,
):
    tokens, columns = queries.shape
    heads = decay_log.shape[1]
    lanes = columns // heads
    blocks = lax.axis_size("seq")
    near = heads
    far = blocks // near
    experts = lax.axis_size("exp")
    copies = lax.axis_size("rep")
    owners = experts * copies
    width = columns * owners
    half_cap = CAP // copies
    near_groups = [[near * i + k for k in range(near)] for i in range(far)]
    far_groups = [[i + near * k for k in range(far)] for i in range(near)]
    near_all = [[m * owners + j for m in group for j in range(owners)] for group in near_groups]

    def by_head(x):
        return jnp.swapaxes(x.reshape(tokens, heads, lanes), 0, 1)

    cumulative = jnp.cumsum(decay_log, axis=0)
    terms = jnp.swapaxes(three_terms(cumulative), 0, 2)
    terms = jnp.swapaxes(terms, 1, 2)
    terms = jnp.pad(terms, ((0, 0), (0, 5), (0, lanes - tokens)))
    payload = jnp.concatenate(
        [by_head(queries), by_head(key_rows), by_head(value_rows), terms], axis=1
    )
    arrived = lax.all_to_all(payload, "seq", 0, 0, tiled=True, axis_index_groups=near_groups)
    span = near * tokens
    query = arrived[:, :tokens].reshape(span, lanes)
    key = arrived[:, tokens : 2 * tokens].reshape(span, lanes)
    value = arrived[:, 2 * tokens : 3 * tokens].reshape(span, lanes)
    within = arrived[:, 3 * tokens : 3 * tokens + 3, :tokens].astype(F32).sum(axis=1)
    ends = within[:, -1]
    starts = jnp.cumsum(ends) - ends
    total = jnp.sum(ends)
    cum = (within + starts[:, None]).reshape(span)
    faded = (key.astype(F32) * jnp.exp(total - cum)[:, None]).astype(BF16)
    state = lax.dot_general(faded, value, (((0,), (0,)), ((), ())), preferred_element_type=F32)
    my_far = lax.axis_index("seq") // near
    fade = jnp.exp(total)
    first = state.astype(BF16)
    order = sorted(range(1, far), key=lambda g: (g != 1, min(g, far - g), -g))
    from_first = []
    for g in order:
        from_first.append(
            lax.ppermute(first, "seq", [(i, near * g + i) for i in range(near)])
        )
    scales = jnp.exp2(jnp.arange(8, dtype=F32) / 8)[:, None]
    scales = jnp.broadcast_to(scales, (8, lanes))
    own = jnp.pad(state, ((0, 8), (0, 0)))
    opening = jnp.where(my_far <= 1, scales, 0.0)
    carried = jnp.pad(opening, ((lanes, 0), (0, 0)))
    for k in range(1, far - 1):
        running = (fade * carried + own).astype(BF16)
        passed = [(near * k + i, near * (k + 1) + i) for i in range(near)]
        received = lax.ppermute(running, "seq", passed)
        carried = carried + received.astype(F32)
    factor = jnp.mean(carried[lanes:] / scales, axis=0)
    from_first = sum(x.astype(F32) for x in from_first)
    incoming = carried[:lanes] + factor * from_first
    scores = lax.dot_general(query, key, (((1,), (1,)), ((), ())), preferred_element_type=F32)
    places = jnp.arange(span)
    causal = places[:, None] >= places[None, :]
    decays = jnp.where(causal, jnp.exp(jnp.where(causal, cum[:, None] - cum[None, :], 0.0)), 0.0)
    mixing = (scores * decays).astype(BF16)
    lifted = (query.astype(F32) * jnp.exp(cum)[:, None]).astype(BF16)
    local_part = lax.optimization_barrier(
        jnp.dot(mixing, value, preferred_element_type=F32)
    )
    attended = local_part + jnp.dot(lifted, incoming.astype(BF16), preferred_element_type=F32)
    attended = attended.astype(BF16).reshape(near, tokens, lanes)
    attended = lax.all_to_all(attended, "seq", 0, 0, tiled=True, axis_index_groups=near_groups)
    attended = jnp.swapaxes(attended, 0, 1).reshape(tokens, columns).astype(F32)

    sumsq = jnp.sum(attended * attended, axis=1)
    branch = jax.nn.sigmoid(out_gate.astype(F32)) * attended * attn_gain
    dispatch, combine = slot_tables(routes, route_weights, experts, CAP)
    both = jnp.concatenate([residual, branch.astype(BF16)], axis=1)
    packed = jnp.dot(jnp.transpose(dispatch).astype(BF16), both, preferred_element_type=F32)
    packed = packed.astype(BF16).reshape(owners, half_cap * 2 * heads, lanes)
    sums = jnp.pad(three_terms(sumsq), ((0, 0), (0, lanes - tokens)))
    gains = three_terms(moe_gain).reshape(3 * heads, lanes)
    extra = jnp.concatenate([sums, gains], axis=0)
    extra = padded_rows(extra, 16)
    extra = jnp.broadcast_to(extra[None], (owners, *extra.shape))
    payload = jnp.concatenate([packed, extra], axis=1)
    arrived = lax.all_to_all(payload, ("exp", "rep"), 0, 0, tiled=True)
    size = half_cap * 2 * heads
    rows = arrived[:, :size].reshape(owners, half_cap, 2, columns).astype(F32)
    sums = arrived[:, size : size + 3, :tokens].astype(F32).sum(axis=(0, 1))
    gains = arrived[:, size + 3 : size + 3 + 3 * heads].astype(F32)
    gains = gains.reshape(owners, 3, columns).sum(axis=1)
    attn_scale = lax.rsqrt(sums / width + EPSILON)
    me = lax.axis_index(("exp", "rep"))
    mine = lax.dynamic_slice_in_dim(dispatch, me * half_cap, half_cap, axis=1)
    slot_scale = jnp.sum(mine * attn_scale[:, None], axis=0)
    slot_hidden = rows[:, :, 0] + slot_scale[None, :, None] * rows[:, :, 1]
    moe_sumsq = jnp.sum(slot_hidden * slot_hidden, axis=(0, 2))
    moe_scale = lax.rsqrt(moe_sumsq / width + EPSILON)
    normed = (slot_hidden * moe_scale[None, :, None] * gains[:, None, :]).astype(BF16)
    normed = jnp.swapaxes(normed, 0, 1).reshape(half_cap * width // lanes, lanes)

    gathered = lax.all_gather(normed, "seq", axis=0, tiled=True, axis_index_groups=far_groups)
    gathered = lax.all_gather(gathered, "seq", axis=0, tiled=True, axis_index_groups=near_groups)
    slot_rows = gathered.reshape(blocks * half_cap, width)
    gate_val = project_rows(slot_rows, w_gate[0])
    up_val = project_rows(slot_rows, w_up[0])
    inner = (jax.nn.silu(gate_val) * up_val).astype(BF16)
    partial = jnp.dot(inner, w_down[0], preferred_element_type=F32).astype(BF16)
    pieces = partial.reshape(near, far * half_cap, owners, columns)
    pieces = jnp.swapaxes(pieces, 1, 2).reshape(near * owners, far * half_cap, columns)
    pieces = lax.all_to_all(
        pieces, ("seq", "exp", "rep"), 0, 0, tiled=True, axis_index_groups=near_all
    )
    pieces = pieces.reshape(near, owners, far, half_cap, columns).astype(F32).sum(axis=0)
    pieces = jnp.swapaxes(pieces.astype(BF16), 0, 1).reshape(far, owners * half_cap, columns)
    pieces = lax.all_to_all(pieces, "seq", 0, 0, tiled=True, axis_index_groups=far_groups)
    returned = pieces.astype(F32).sum(axis=0).astype(BF16)
    expert_mix = jnp.dot(combine, returned.astype(F32), precision=lax.Precision.HIGHEST)
    hidden = residual.astype(F32) + attn_scale[:, None] * branch
    return (hidden + expert_mix).astype(BF16)


def solution(mesh):
    return jax.shard_map(
        shards,
        mesh=mesh,
        in_specs=(
            P(("groups", "seq"), ("exp", "rep")),
            P(("groups", "seq"), ("exp", "rep")),
            P(("groups", "seq"), ("exp", "rep")),
            P(("groups", "seq"), ("exp", "rep")),
            P(("groups", "seq"), ("exp", "rep")),
            P(("groups", "seq"), ("exp", "rep")),
            P(("exp", "rep")),
            P(("exp", "rep")),
            P(("groups", "seq"), None),
            P(("groups", "seq"), None),
            P("exp", "seq", None),
            P("exp", "seq", None),
            P("exp", "seq", None),
        ),
        out_specs=P(("groups", "seq"), ("exp", "rep")),
        check_vma=False,
    )
```

```python
from functools import partial

import jax
import jax.numpy as jnp
from jax import lax
from jax.experimental import pallas as pl
from jax.experimental.pallas import tpu as pltpu
from jax.sharding import PartitionSpec as P

CAP = 6


EPSILON = 1e-06

F32 = jnp.float32
BF16 = jnp.bfloat16


def three_terms(x):
    high = lax.reduce_precision(x, 8, 7)
    rest = x - high
    middle = lax.reduce_precision(rest, 8, 7)
    low = rest - middle
    return jnp.stack([high, middle, low]).astype(BF16)


def slot_tables(route_block, weight_block, experts, capacity):
    expert_ids = jnp.arange(experts, dtype=jnp.int32)
    onehot = (route_block[:, :, None] == expert_ids[None, None, :]).astype(jnp.int32)
    tokens = route_block.shape[0]
    flat_hits = onehot.reshape(tokens * 2, experts)
    before = jnp.cumsum(flat_hits, axis=0) - flat_hits
    places = jnp.arange(capacity, dtype=jnp.int32)
    hit_table = flat_hits[:, :, None] * (before[:, :, None] == places[None, None, :]).astype(
        jnp.int32
    )
    hit_table = hit_table.astype(jnp.float32).reshape(tokens, 2, experts * capacity)
    dispatch = jnp.sum(hit_table, axis=1)
    combine = jnp.sum(hit_table * weight_block[:, :, None], axis=1)
    return (dispatch, combine)


def padded_rows(x, rows):
    return jnp.pad(x, [(0, 0)] * (x.ndim - 2) + [(0, rows - x.shape[-2]), (0, 0)])


def rounded(x):
    return x.astype(BF16).astype(F32)


def payload_body(
    query_hbm, key_hbm, value_hbm, decay_hbm, out_ref, query_ref, key_ref, value_ref, decay_ref, arrivals
):
    fetches = [
        pltpu.make_async_copy(source, target, arrivals.at[i])
        for i, (source, target) in enumerate(
            [
                (decay_hbm, decay_ref),
                (query_hbm, query_ref),
                (key_hbm, key_ref),
                (value_hbm, value_ref),
            ]
        )
    ]
    for fetch in fetches:
        fetch.start()
    tokens, columns = query_ref.shape
    heads = out_ref.shape[0]
    lanes = columns // heads
    row = lax.broadcasted_iota(jnp.int32, (tokens, lanes), 0)
    col = lax.broadcasted_iota(jnp.int32, (tokens, lanes), 1)
    upto = jnp.where((row <= col) & (col < tokens), 1.0, 0.0)
    fetches[0].wait()
    cumulative = jnp.dot(
        decay_ref[...], upto, precision=lax.Precision.HIGHEST, preferred_element_type=F32
    )
    high = rounded(cumulative)
    middle = rounded(cumulative - high)
    low = cumulative - high - middle
    place = lax.broadcasted_iota(jnp.int32, (8, lanes), 0)
    for fetch in fetches[1:]:
        fetch.wait()
    for h in range(heads):
        here = slice(h * lanes, (h + 1) * lanes)
        out_ref[h, :tokens] = query_ref[:, here]
        out_ref[h, tokens : 2 * tokens] = key_ref[:, here]
        out_ref[h, 2 * tokens : 3 * tokens] = value_ref[:, here]
        tail = jnp.where(place == 0, high[h : h + 1], 0.0)
        tail = jnp.where(place == 1, middle[h : h + 1], tail)
        tail = jnp.where(place == 2, low[h : h + 1], tail)
        out_ref[h, 3 * tokens :] = tail.astype(BF16)


def state_body(tokens, arrived_ref, state_ref, fade_ref):
    near, _, lanes = arrived_ref.shape
    sums = [
        jnp.sum(arrived_ref[b, 3 * tokens :].astype(F32), axis=0, keepdims=True)
        for b in range(near)
    ]
    ends = [x[:, tokens - 1 : tokens] for x in sums]
    left = jnp.zeros_like(ends[0])
    state = jnp.zeros((lanes, lanes), F32)
    for b in reversed(range(near)):
        left = left + ends[b]
        weight = jnp.exp(left - sums[b][:, :tokens])
        key = jnp.transpose(arrived_ref[b, tokens : 2 * tokens].astype(F32))
        state = state + jnp.dot(
            (key * weight).astype(BF16),
            arrived_ref[b, 2 * tokens : 3 * tokens],
            preferred_element_type=F32,
        )
    state_ref[...] = state
    fade_ref[...] = jnp.broadcast_to(jnp.exp(left), fade_ref.shape)


def expert_body(near, rows_ref, gate_ref, up_ref, down_hbm, out_ref, down_ref, arrival):
    pieces, height, columns = out_ref.shape
    fetch = pltpu.make_async_copy(down_hbm, down_ref, arrival)
    fetch.start()
    owners = pieces // near
    contract = (((1,), (1,)), ((), ()))
    rows = rows_ref[...]
    gate = lax.dot_general(rows, gate_ref[0], contract, preferred_element_type=F32)
    up = lax.dot_general(rows, up_ref[0], contract, preferred_element_type=F32)
    inner = (gate / (1.0 + jnp.exp(-gate)) * up).astype(BF16)
    fetch.wait()
    for j in range(owners):
        part = jnp.dot(
            inner,
            down_ref[0, :, j * columns : (j + 1) * columns],
            preferred_element_type=F32,
        ).astype(BF16)
        for r in range(near):
            out_ref[r * owners + j] = part[r * height : (r + 1) * height]


SMALL = pltpu.CompilerParams(vmem_limit_bytes=4 * 1024 * 1024)


def whole(count):
    return [pl.BlockSpec(memory_space=pltpu.VMEM)] * count


def shards(
    queries,
    key_rows,
    value_rows,
    decay_log,
    residual,
    out_gate,
    attn_gain,
    moe_gain,
    routes,
    route_weights,
    w_gate,
    w_up,
    w_down,
):
    tokens, columns = queries.shape
    heads = decay_log.shape[1]
    lanes = columns // heads
    blocks = lax.axis_size("seq")
    near = heads
    far = blocks // near
    experts = lax.axis_size("exp")
    copies = lax.axis_size("rep")
    owners = experts * copies
    width = columns * owners
    half_cap = CAP // copies
    near_groups = [[near * i + k for k in range(near)] for i in range(far)]
    far_groups = [[i + near * k for k in range(far)] for i in range(near)]
    near_all = [[m * owners + j for m in group for j in range(owners)] for group in near_groups]

    payload = pl.pallas_call(
        payload_body,
        out_shape=jax.ShapeDtypeStruct((heads, 3 * tokens + 8, lanes), BF16),
        in_specs=[pl.BlockSpec(memory_space=pl.ANY)] * 4,
        out_specs=whole(1)[0],
        scratch_shapes=[
            *[pltpu.VMEM((tokens, columns), BF16)] * 3,
            pltpu.VMEM((heads, tokens), F32),
            pltpu.SemaphoreType.DMA((4,)),
        ],
        name="payload",
    )(queries, key_rows, value_rows, jnp.transpose(decay_log))
    arrived = lax.all_to_all(payload, "seq", 0, 0, tiled=True, axis_index_groups=near_groups)
    span = near * tokens
    query = arrived[:, :tokens].reshape(span, lanes)
    key = arrived[:, tokens : 2 * tokens].reshape(span, lanes)
    value = arrived[:, 2 * tokens : 3 * tokens].reshape(span, lanes)
    within = arrived[:, 3 * tokens : 3 * tokens + 3, :tokens].astype(F32).sum(axis=1)
    ends = within[:, -1]
    starts = jnp.cumsum(ends) - ends
    cum = (within + starts[:, None]).reshape(span)
    state, fade = pl.pallas_call(
        partial(state_body, tokens),
        out_shape=(
            jax.ShapeDtypeStruct((lanes, lanes), F32),
            jax.ShapeDtypeStruct((8, lanes), F32),
        ),
        in_specs=whole(1),
        out_specs=tuple(whole(2)),
        compiler_params=SMALL,
        name="group_state",
    )(arrived)
    fade = fade[:1]
    my_far = lax.axis_index("seq") // near
    first = state.astype(BF16)
    order = sorted(range(1, far), key=lambda g: (g != 1, min(g, far - g), -g))
    from_first = []
    for g in order:
        from_first.append(
            lax.ppermute(first, "seq", [(i, near * g + i) for i in range(near)])
        )
    scales = jnp.exp2(jnp.arange(8, dtype=F32) / 8)[:, None]
    scales = jnp.broadcast_to(scales, (8, lanes))
    own = jnp.pad(state, ((0, 8), (0, 0)))
    opening = jnp.where(my_far <= 1, scales, 0.0)
    carried = jnp.pad(opening, ((lanes, 0), (0, 0)))
    for k in range(1, far - 1):
        running = (fade * carried + own).astype(BF16)
        passed = [(near * k + i, near * (k + 1) + i) for i in range(near)]
        received = lax.ppermute(running, "seq", passed)
        carried = carried + received.astype(F32)
    factor = jnp.mean(carried[lanes:] / scales, axis=0)
    from_first = sum(x.astype(F32) for x in from_first)
    incoming = carried[:lanes] + factor * from_first
    scores = lax.dot_general(query, key, (((1,), (1,)), ((), ())), preferred_element_type=F32)
    places = jnp.arange(span)
    causal = places[:, None] >= places[None, :]
    decays = jnp.where(causal, jnp.exp(jnp.where(causal, cum[:, None] - cum[None, :], 0.0)), 0.0)
    mixing = (scores * decays).astype(BF16)
    lifted = (query.astype(F32) * jnp.exp(cum)[:, None]).astype(BF16)
    local_part = lax.optimization_barrier(
        jnp.dot(mixing, value, preferred_element_type=F32)
    )
    attended = local_part + jnp.dot(lifted, incoming.astype(BF16), preferred_element_type=F32)
    attended = attended.astype(BF16).reshape(near, tokens, lanes)
    attended = lax.all_to_all(attended, "seq", 0, 0, tiled=True, axis_index_groups=near_groups)
    attended = jnp.swapaxes(attended, 0, 1).reshape(tokens, columns).astype(F32)

    sumsq = jnp.sum(attended * attended, axis=1)
    branch = jax.nn.sigmoid(out_gate.astype(F32)) * attended * attn_gain
    dispatch, combine = slot_tables(routes, route_weights, experts, CAP)
    both = jnp.concatenate([residual, branch.astype(BF16)], axis=1)
    packed = jnp.dot(jnp.transpose(dispatch).astype(BF16), both, preferred_element_type=F32)
    packed = packed.astype(BF16).reshape(owners, half_cap * 2 * heads, lanes)
    sums = jnp.pad(three_terms(sumsq), ((0, 0), (0, lanes - tokens)))
    gains = three_terms(moe_gain).reshape(3 * heads, lanes)
    extra = jnp.concatenate([sums, gains], axis=0)
    extra = padded_rows(extra, 16)
    extra = jnp.broadcast_to(extra[None], (owners, *extra.shape))
    payload = jnp.concatenate([packed, extra], axis=1)
    arrived = lax.all_to_all(payload, ("exp", "rep"), 0, 0, tiled=True)
    size = half_cap * 2 * heads
    rows = arrived[:, :size].reshape(owners, half_cap, 2, columns).astype(F32)
    sums = arrived[:, size : size + 3, :tokens].astype(F32).sum(axis=(0, 1))
    gains = arrived[:, size + 3 : size + 3 + 3 * heads].astype(F32)
    gains = gains.reshape(owners, 3, columns).sum(axis=1)
    attn_scale = lax.rsqrt(sums / width + EPSILON)
    me = lax.axis_index(("exp", "rep"))
    mine = lax.dynamic_slice_in_dim(dispatch, me * half_cap, half_cap, axis=1)
    slot_scale = jnp.sum(mine * attn_scale[:, None], axis=0)
    slot_hidden = rows[:, :, 0] + slot_scale[None, :, None] * rows[:, :, 1]
    moe_sumsq = jnp.sum(slot_hidden * slot_hidden, axis=(0, 2))
    moe_scale = lax.rsqrt(moe_sumsq / width + EPSILON)
    normed = (slot_hidden * moe_scale[None, :, None] * gains[:, None, :]).astype(BF16)
    normed = jnp.swapaxes(normed, 0, 1).reshape(half_cap * width // lanes, lanes)

    gathered = lax.all_gather(normed, "seq", axis=0, tiled=True, axis_index_groups=far_groups)
    gathered = lax.all_gather(gathered, "seq", axis=0, tiled=True, axis_index_groups=near_groups)
    slot_rows = gathered.reshape(blocks * half_cap, width)
    pieces = pl.pallas_call(
        partial(expert_body, near),
        out_shape=jax.ShapeDtypeStruct((near * owners, far * half_cap, columns), BF16),
        in_specs=[*whole(3), pl.BlockSpec(memory_space=pl.ANY)],
        out_specs=whole(1)[0],
        scratch_shapes=[pltpu.VMEM(w_down.shape, BF16), pltpu.SemaphoreType.DMA],
        compiler_params=pltpu.CompilerParams(vmem_limit_bytes=52_500_000),
        name="experts",
    )(slot_rows, w_gate, w_up, w_down)
    pieces = lax.all_to_all(
        pieces, ("seq", "exp", "rep"), 0, 0, tiled=True, axis_index_groups=near_all
    )
    pieces = pieces.reshape(near, owners, far, half_cap, columns).astype(F32).sum(axis=0)
    pieces = jnp.swapaxes(pieces.astype(BF16), 0, 1).reshape(far, owners * half_cap, columns)
    pieces = lax.all_to_all(pieces, "seq", 0, 0, tiled=True, axis_index_groups=far_groups)
    returned = pieces.astype(F32).sum(axis=0).astype(BF16)
    expert_mix = jnp.dot(combine, returned.astype(F32), precision=lax.Precision.HIGHEST)
    hidden = residual.astype(F32) + attn_scale[:, None] * branch
    return (hidden + expert_mix).astype(BF16)


def solution(mesh):
    return jax.shard_map(
        shards,
        mesh=mesh,
        in_specs=(
            P(("groups", "seq"), ("exp", "rep")),
            P(("groups", "seq"), ("exp", "rep")),
            P(("groups", "seq"), ("exp", "rep")),
            P(("groups", "seq"), ("exp", "rep")),
            P(("groups", "seq"), ("exp", "rep")),
            P(("groups", "seq"), ("exp", "rep")),
            P(("exp", "rep")),
            P(("exp", "rep")),
            P(("groups", "seq"), None),
            P(("groups", "seq"), None),
            P("exp", "seq", None),
            P("exp", "seq", None),
            P("exp", "seq", None),
        ),
        out_specs=P(("groups", "seq"), ("exp", "rep")),
        check_vma=False,
    )
```

```python
from functools import partial

import jax
import jax.numpy as jnp
from jax import lax
from jax.experimental import pallas as pl
from jax.experimental.pallas import tpu as pltpu
from jax.sharding import PartitionSpec as P

CAP = 6


EPSILON = 1e-06

F32 = jnp.float32
BF16 = jnp.bfloat16


def three_terms(x):
    high = lax.reduce_precision(x, 8, 7)
    rest = x - high
    middle = lax.reduce_precision(rest, 8, 7)
    low = rest - middle
    return jnp.stack([high, middle, low]).astype(BF16)


def slot_tables(route_block, weight_block, experts, capacity):
    expert_ids = jnp.arange(experts, dtype=jnp.int32)
    onehot = (route_block[:, :, None] == expert_ids[None, None, :]).astype(jnp.int32)
    tokens = route_block.shape[0]
    flat_hits = onehot.reshape(tokens * 2, experts)
    before = jnp.cumsum(flat_hits, axis=0) - flat_hits
    places = jnp.arange(capacity, dtype=jnp.int32)
    hit_table = flat_hits[:, :, None] * (before[:, :, None] == places[None, None, :]).astype(
        jnp.int32
    )
    hit_table = hit_table.astype(jnp.float32).reshape(tokens, 2, experts * capacity)
    dispatch = jnp.sum(hit_table, axis=1)
    combine = jnp.sum(hit_table * weight_block[:, :, None], axis=1)
    return (dispatch, combine)


def padded_rows(x, rows):
    return jnp.pad(x, [(0, 0)] * (x.ndim - 2) + [(0, rows - x.shape[-2]), (0, 0)])


def rounded(x):
    return x.astype(BF16).astype(F32)


def payload_body(
    query_hbm, key_hbm, value_hbm, decay_hbm, out_ref, query_ref, key_ref, value_ref, decay_ref, arrivals
):
    fetches = [
        pltpu.make_async_copy(source, target, arrivals.at[i])
        for i, (source, target) in enumerate(
            [
                (decay_hbm, decay_ref),
                (query_hbm, query_ref),
                (key_hbm, key_ref),
                (value_hbm, value_ref),
            ]
        )
    ]
    for fetch in fetches:
        fetch.start()
    tokens, columns = query_ref.shape
    heads = out_ref.shape[0]
    lanes = columns // heads
    row = lax.broadcasted_iota(jnp.int32, (tokens, lanes), 0)
    col = lax.broadcasted_iota(jnp.int32, (tokens, lanes), 1)
    upto = jnp.where((row <= col) & (col < tokens), 1.0, 0.0)
    fetches[0].wait()
    cumulative = jnp.dot(
        decay_ref[...], upto, precision=lax.Precision.HIGHEST, preferred_element_type=F32
    )
    high = rounded(cumulative)
    middle = rounded(cumulative - high)
    low = cumulative - high - middle
    place = lax.broadcasted_iota(jnp.int32, (8, lanes), 0)
    for fetch in fetches[1:]:
        fetch.wait()
    for h in range(heads):
        here = slice(h * lanes, (h + 1) * lanes)
        out_ref[h, :tokens] = query_ref[:, here]
        out_ref[h, tokens : 2 * tokens] = key_ref[:, here]
        out_ref[h, 2 * tokens : 3 * tokens] = value_ref[:, here]
        tail = jnp.where(place == 0, high[h : h + 1], 0.0)
        tail = jnp.where(place == 1, middle[h : h + 1], tail)
        tail = jnp.where(place == 2, low[h : h + 1], tail)
        out_ref[h, 3 * tokens :] = tail.astype(BF16)


def state_body(tokens, arrived_ref, state_ref, fade_ref, own_ref):
    near, _, lanes = arrived_ref.shape
    sums = [
        jnp.sum(arrived_ref[b, 3 * tokens :].astype(F32), axis=0, keepdims=True)
        for b in range(near)
    ]
    ends = [x[:, tokens - 1 : tokens] for x in sums]
    left = jnp.zeros_like(ends[0])
    state = jnp.zeros((lanes, lanes), F32)
    for b in reversed(range(near)):
        left = left + ends[b]
        weight = jnp.exp(left - sums[b][:, :tokens])
        key = jnp.transpose(arrived_ref[b, tokens : 2 * tokens].astype(F32))
        state = state + jnp.dot(
            (key * weight).astype(BF16),
            arrived_ref[b, 2 * tokens : 3 * tokens],
            preferred_element_type=F32,
        )
    state_ref[...] = state
    fade = jnp.broadcast_to(jnp.exp(left), fade_ref.shape)
    fade_ref[...] = fade
    high = rounded(fade)
    middle = rounded(fade - high)
    place = lax.broadcasted_iota(jnp.int32, fade.shape, 0)
    tail = jnp.where(place == 2, fade - high - middle, 0.0)
    tail = jnp.where(place == 1, middle, tail)
    tail = jnp.where(place == 0, high, tail)
    own_ref[:lanes] = state.astype(BF16)
    own_ref[lanes:] = tail.astype(BF16)


def expert_body(
    near, rows_ref, gate_hbm, up_hbm, down_hbm, out_ref, gate_ref, up_ref, down_ref, arrivals
):
    pieces, height, columns = out_ref.shape
    fetches = [
        pltpu.make_async_copy(source, target, arrivals.at[i])
        for i, (source, target) in enumerate(
            [(gate_hbm, gate_ref), (up_hbm, up_ref), (down_hbm, down_ref)]
        )
    ]
    for fetch in fetches:
        fetch.start()
    owners = pieces // near
    contract = (((1,), (1,)), ((), ()))
    rows = rows_ref[...]
    fetches[0].wait()
    gate = lax.dot_general(rows, gate_ref[0], contract, preferred_element_type=F32)
    fetches[1].wait()
    up = lax.dot_general(rows, up_ref[0], contract, preferred_element_type=F32)
    inner = (gate / (1.0 + jnp.exp(-gate)) * up).astype(BF16)
    fetches[2].wait()
    for j in range(owners):
        part = jnp.dot(
            inner,
            down_ref[0, :, j * columns : (j + 1) * columns],
            preferred_element_type=F32,
        ).astype(BF16)
        for r in range(near):
            out_ref[r * owners + j] = part[r * height : (r + 1) * height]


SMALL = pltpu.CompilerParams(vmem_limit_bytes=4 * 1024 * 1024)


def whole(count):
    return [pl.BlockSpec(memory_space=pltpu.VMEM)] * count


def shards(
    queries,
    key_rows,
    value_rows,
    decay_log,
    residual,
    out_gate,
    attn_gain,
    moe_gain,
    routes,
    route_weights,
    w_gate,
    w_up,
    w_down,
):
    tokens, columns = queries.shape
    heads = decay_log.shape[1]
    lanes = columns // heads
    blocks = lax.axis_size("seq")
    near = heads
    far = blocks // near
    experts = lax.axis_size("exp")
    copies = lax.axis_size("rep")
    owners = experts * copies
    width = columns * owners
    half_cap = CAP // copies
    near_groups = [[near * i + k for k in range(near)] for i in range(far)]
    far_groups = [[i + near * k for k in range(far)] for i in range(near)]
    near_all = [[m * owners + j for m in group for j in range(owners)] for group in near_groups]

    payload = pl.pallas_call(
        payload_body,
        out_shape=jax.ShapeDtypeStruct((heads, 3 * tokens + 8, lanes), BF16),
        in_specs=[pl.BlockSpec(memory_space=pl.ANY)] * 4,
        out_specs=whole(1)[0],
        scratch_shapes=[
            *[pltpu.VMEM((tokens, columns), BF16)] * 3,
            pltpu.VMEM((heads, tokens), F32),
            pltpu.SemaphoreType.DMA((4,)),
        ],
        name="payload",
    )(queries, key_rows, value_rows, jnp.transpose(decay_log))
    arrived = lax.all_to_all(payload, "seq", 0, 0, tiled=True, axis_index_groups=near_groups)
    span = near * tokens
    query = arrived[:, :tokens].reshape(span, lanes)
    key = arrived[:, tokens : 2 * tokens].reshape(span, lanes)
    value = arrived[:, 2 * tokens : 3 * tokens].reshape(span, lanes)
    within = arrived[:, 3 * tokens : 3 * tokens + 3, :tokens].astype(F32).sum(axis=1)
    ends = within[:, -1]
    starts = jnp.cumsum(ends) - ends
    cum = (within + starts[:, None]).reshape(span)
    state, fade, own = pl.pallas_call(
        partial(state_body, tokens),
        out_shape=(
            jax.ShapeDtypeStruct((lanes, lanes), F32),
            jax.ShapeDtypeStruct((8, lanes), F32),
            jax.ShapeDtypeStruct((lanes + 8, lanes), BF16),
        ),
        in_specs=whole(1),
        out_specs=tuple(whole(3)),
        compiler_params=SMALL,
        name="group_state",
    )(arrived)
    fade = fade[:1]
    my_far = lax.axis_index("seq") // near

    def passed(x, pairs):
        return lax.ppermute(
            x, "seq", [(near * p + i, near * q + i) for p, q in pairs for i in range(near)]
        )

    early = [(1, 2)] + [(g, g + 1) for g in range(4, far, 2)]
    beside = passed(own, early)
    first = own[:lanes]
    order = sorted(range(1, far), key=lambda g: (g != 1, min(g, far - g), -g))
    from_first = []
    for g in order:
        from_first.append(passed(first, [(0, g)]))
    joined = (my_far == 2) | ((my_far >= 5) & (my_far % 2 == 1))
    beside = beside.astype(F32)
    step = jnp.where(joined, beside[lanes] + beside[lanes + 1] + beside[lanes + 2], 1.0)[None]
    scales = jnp.exp2(jnp.arange(8, dtype=F32) / 8)[:, None]
    scales = jnp.broadcast_to(scales, (8, lanes))
    carried = jnp.pad(jnp.where(my_far <= 2, scales, 0.0), ((lanes, 0), (0, 0)))
    slope = fade * step
    offset = jnp.pad(fade * beside[:lanes] + state, ((0, 8), (0, 0)))
    running = (slope * carried + offset).astype(BF16)
    carried = carried + passed(running, [(2, 3)]).astype(F32)
    for g in range(3, far - 1, 2):
        running = (slope * carried + offset).astype(BF16)
        close = passed(running, [(g, g + 1)])
        distant = passed(running, [(g, g + 2)])
        carried = carried + close.astype(F32) + distant.astype(F32)
    factor = jnp.mean(step * carried[lanes:] / scales, axis=0)
    from_first = sum(x.astype(F32) for x in from_first)
    incoming = step * carried[:lanes] + beside[:lanes] + factor * from_first
    scores = lax.dot_general(query, key, (((1,), (1,)), ((), ())), preferred_element_type=F32)
    places = jnp.arange(span)
    causal = places[:, None] >= places[None, :]
    decays = jnp.where(causal, jnp.exp(jnp.where(causal, cum[:, None] - cum[None, :], 0.0)), 0.0)
    mixing = (scores * decays).astype(BF16)
    lifted = (query.astype(F32) * jnp.exp(cum)[:, None]).astype(BF16)
    local_part = lax.optimization_barrier(
        jnp.dot(mixing, value, preferred_element_type=F32)
    )
    attended = local_part + jnp.dot(lifted, incoming.astype(BF16), preferred_element_type=F32)
    attended = attended.astype(BF16).reshape(near, tokens, lanes)
    attended = lax.all_to_all(attended, "seq", 0, 0, tiled=True, axis_index_groups=near_groups)
    attended = jnp.swapaxes(attended, 0, 1).reshape(tokens, columns).astype(F32)

    sumsq = jnp.sum(attended * attended, axis=1)
    branch = jax.nn.sigmoid(out_gate.astype(F32)) * attended * attn_gain
    dispatch, combine = slot_tables(routes, route_weights, experts, CAP)
    both = jnp.concatenate([residual, branch.astype(BF16)], axis=1)
    packed = jnp.dot(jnp.transpose(dispatch).astype(BF16), both, preferred_element_type=F32)
    packed = packed.astype(BF16).reshape(owners, half_cap * 2 * heads, lanes)
    sums = jnp.pad(three_terms(sumsq), ((0, 0), (0, lanes - tokens)))
    gains = three_terms(moe_gain).reshape(3 * heads, lanes)
    extra = jnp.concatenate([sums, gains], axis=0)
    extra = padded_rows(extra, 16)
    extra = jnp.broadcast_to(extra[None], (owners, *extra.shape))
    payload = jnp.concatenate([packed, extra], axis=1)
    arrived = lax.all_to_all(payload, ("exp", "rep"), 0, 0, tiled=True)
    size = half_cap * 2 * heads
    rows = arrived[:, :size].reshape(owners, half_cap, 2, columns).astype(F32)
    sums = arrived[:, size : size + 3, :tokens].astype(F32).sum(axis=(0, 1))
    gains = arrived[:, size + 3 : size + 3 + 3 * heads].astype(F32)
    gains = gains.reshape(owners, 3, columns).sum(axis=1)
    attn_scale = lax.rsqrt(sums / width + EPSILON)
    me = lax.axis_index(("exp", "rep"))
    mine = lax.dynamic_slice_in_dim(dispatch, me * half_cap, half_cap, axis=1)
    slot_scale = jnp.sum(mine * attn_scale[:, None], axis=0)
    slot_hidden = rows[:, :, 0] + slot_scale[None, :, None] * rows[:, :, 1]
    moe_sumsq = jnp.sum(slot_hidden * slot_hidden, axis=(0, 2))
    moe_scale = lax.rsqrt(moe_sumsq / width + EPSILON)
    normed = (slot_hidden * moe_scale[None, :, None] * gains[:, None, :]).astype(BF16)
    normed = jnp.swapaxes(normed, 0, 1).reshape(half_cap * width // lanes, lanes)

    gathered = lax.all_gather(normed, "seq", axis=0, tiled=True, axis_index_groups=far_groups)
    gathered = lax.all_gather(gathered, "seq", axis=0, tiled=True, axis_index_groups=near_groups)
    slot_rows = gathered.reshape(blocks * half_cap, width)
    pieces = pl.pallas_call(
        partial(expert_body, near),
        out_shape=jax.ShapeDtypeStruct((near * owners, far * half_cap, columns), BF16),
        in_specs=[*whole(1), *[pl.BlockSpec(memory_space=pl.ANY)] * 3],
        out_specs=whole(1)[0],
        scratch_shapes=[
            *[pltpu.VMEM(w.shape, BF16) for w in (w_gate, w_up, w_down)],
            pltpu.SemaphoreType.DMA((3,)),
        ],
        compiler_params=pltpu.CompilerParams(vmem_limit_bytes=54_000_000),
        name="experts",
    )(slot_rows, w_gate, w_up, w_down)
    pieces = lax.all_to_all(
        pieces, ("seq", "exp", "rep"), 0, 0, tiled=True, axis_index_groups=near_all
    )
    pieces = pieces.reshape(near, owners, far, half_cap, columns).astype(F32).sum(axis=0)
    pieces = jnp.swapaxes(pieces.astype(BF16), 0, 1).reshape(far, owners * half_cap, columns)
    pieces = lax.all_to_all(pieces, "seq", 0, 0, tiled=True, axis_index_groups=far_groups)
    returned = pieces.astype(F32).sum(axis=0).astype(BF16)
    expert_mix = jnp.dot(combine, returned.astype(F32), precision=lax.Precision.HIGHEST)
    hidden = residual.astype(F32) + attn_scale[:, None] * branch
    return (hidden + expert_mix).astype(BF16)


def solution(mesh):
    return jax.shard_map(
        shards,
        mesh=mesh,
        in_specs=(
            P(("groups", "seq"), ("exp", "rep")),
            P(("groups", "seq"), ("exp", "rep")),
            P(("groups", "seq"), ("exp", "rep")),
            P(("groups", "seq"), ("exp", "rep")),
            P(("groups", "seq"), ("exp", "rep")),
            P(("groups", "seq"), ("exp", "rep")),
            P(("exp", "rep")),
            P(("exp", "rep")),
            P(("groups", "seq"), None),
            P(("groups", "seq"), None),
            P("exp", "seq", None),
            P("exp", "seq", None),
            P("exp", "seq", None),
        ),
        out_specs=P(("groups", "seq"), ("exp", "rep")),
        check_vma=False,
    )
```

```python
from functools import partial

import jax
import jax.numpy as jnp
from jax import lax
from jax.experimental import pallas as pl
from jax.experimental.pallas import tpu as pltpu
from jax.sharding import PartitionSpec as P

CAP = 6


EPSILON = 1e-06

F32 = jnp.float32
BF16 = jnp.bfloat16


def three_terms(x):
    high = lax.reduce_precision(x, 8, 7)
    rest = x - high
    middle = lax.reduce_precision(rest, 8, 7)
    low = rest - middle
    return jnp.stack([high, middle, low]).astype(BF16)


def slot_tables(route_block, weight_block, experts, capacity):
    expert_ids = jnp.arange(experts, dtype=jnp.int32)
    onehot = (route_block[:, :, None] == expert_ids[None, None, :]).astype(jnp.int32)
    tokens = route_block.shape[0]
    flat_hits = onehot.reshape(tokens * 2, experts)
    before = jnp.cumsum(flat_hits, axis=0) - flat_hits
    places = jnp.arange(capacity, dtype=jnp.int32)
    hit_table = flat_hits[:, :, None] * (before[:, :, None] == places[None, None, :]).astype(
        jnp.int32
    )
    hit_table = hit_table.astype(jnp.float32).reshape(tokens, 2, experts * capacity)
    dispatch = jnp.sum(hit_table, axis=1)
    combine = jnp.sum(hit_table * weight_block[:, :, None], axis=1)
    return (dispatch, combine)


def padded_rows(x, rows):
    return jnp.pad(x, [(0, 0)] * (x.ndim - 2) + [(0, rows - x.shape[-2]), (0, 0)])


def rounded(x):
    return x.astype(BF16).astype(F32)


def payload_body(
    query_hbm, key_hbm, value_hbm, decay_hbm, out_ref, query_ref, key_ref, value_ref, decay_ref, arrivals
):
    fetches = [
        pltpu.make_async_copy(source, target, arrivals.at[i])
        for i, (source, target) in enumerate(
            [
                (decay_hbm, decay_ref),
                (query_hbm, query_ref),
                (key_hbm, key_ref),
                (value_hbm, value_ref),
            ]
        )
    ]
    for fetch in fetches:
        fetch.start()
    tokens, columns = query_ref.shape
    heads = out_ref.shape[0]
    lanes = columns // heads
    row = lax.broadcasted_iota(jnp.int32, (tokens, lanes), 0)
    col = lax.broadcasted_iota(jnp.int32, (tokens, lanes), 1)
    upto = jnp.where((row <= col) & (col < tokens), 1.0, 0.0)
    fetches[0].wait()
    cumulative = jnp.dot(
        decay_ref[...], upto, precision=lax.Precision.HIGHEST, preferred_element_type=F32
    )
    high = rounded(cumulative)
    middle = rounded(cumulative - high)
    low = cumulative - high - middle
    place = lax.broadcasted_iota(jnp.int32, (8, lanes), 0)
    for fetch in fetches[1:]:
        fetch.wait()
    for h in range(heads):
        here = slice(h * lanes, (h + 1) * lanes)
        out_ref[h, :tokens] = query_ref[:, here]
        out_ref[h, tokens : 2 * tokens] = key_ref[:, here]
        out_ref[h, 2 * tokens : 3 * tokens] = value_ref[:, here]
        tail = jnp.where(place == 0, high[h : h + 1], 0.0)
        tail = jnp.where(place == 1, middle[h : h + 1], tail)
        tail = jnp.where(place == 2, low[h : h + 1], tail)
        out_ref[h, 3 * tokens :] = tail.astype(BF16)


def state_body(tokens, arrived_ref, state_ref, fade_ref, own_ref):
    near, _, lanes = arrived_ref.shape
    sums = [
        jnp.sum(arrived_ref[b, 3 * tokens :].astype(F32), axis=0, keepdims=True)
        for b in range(near)
    ]
    ends = [x[:, tokens - 1 : tokens] for x in sums]
    left = jnp.zeros_like(ends[0])
    state = jnp.zeros((lanes, lanes), F32)
    for b in reversed(range(near)):
        left = left + ends[b]
        weight = jnp.exp(left - sums[b][:, :tokens])
        key = jnp.transpose(arrived_ref[b, tokens : 2 * tokens].astype(F32))
        state = state + jnp.dot(
            (key * weight).astype(BF16),
            arrived_ref[b, 2 * tokens : 3 * tokens],
            preferred_element_type=F32,
        )
    state_ref[...] = state
    fade = jnp.broadcast_to(jnp.exp(left), fade_ref.shape)
    fade_ref[...] = fade
    high = rounded(fade)
    middle = rounded(fade - high)
    place = lax.broadcasted_iota(jnp.int32, fade.shape, 0)
    tail = jnp.where(place == 2, fade - high - middle, 0.0)
    tail = jnp.where(place == 1, middle, tail)
    tail = jnp.where(place == 0, high, tail)
    own_ref[:lanes] = state.astype(BF16)
    own_ref[lanes:] = tail.astype(BF16)


def expert_body(near, rows_ref, gate_ref, up_ref, down_hbm, out_ref, down_ref, arrival):
    pieces, height, columns = out_ref.shape
    fetch = pltpu.make_async_copy(down_hbm, down_ref, arrival)
    fetch.start()
    owners = pieces // near
    contract = (((1,), (1,)), ((), ()))
    rows = rows_ref[...]
    gate = lax.dot_general(rows, gate_ref[0], contract, preferred_element_type=F32)
    up = lax.dot_general(rows, up_ref[0], contract, preferred_element_type=F32)
    inner = (gate / (1.0 + jnp.exp(-gate)) * up).astype(BF16)
    fetch.wait()
    for j in range(owners):
        part = jnp.dot(
            inner,
            down_ref[0, :, j * columns : (j + 1) * columns],
            preferred_element_type=F32,
        ).astype(BF16)
        for r in range(near):
            out_ref[r * owners + j] = part[r * height : (r + 1) * height]


SMALL = pltpu.CompilerParams(vmem_limit_bytes=4 * 1024 * 1024)


def whole(count):
    return [pl.BlockSpec(memory_space=pltpu.VMEM)] * count


def shards(
    queries,
    key_rows,
    value_rows,
    decay_log,
    residual,
    out_gate,
    attn_gain,
    moe_gain,
    routes,
    route_weights,
    w_gate,
    w_up,
    w_down,
):
    tokens, columns = queries.shape
    heads = decay_log.shape[1]
    lanes = columns // heads
    blocks = lax.axis_size("seq")
    near = heads
    far = blocks // near
    experts = lax.axis_size("exp")
    copies = lax.axis_size("rep")
    owners = experts * copies
    width = columns * owners
    half_cap = CAP // copies
    near_groups = [[near * i + k for k in range(near)] for i in range(far)]
    far_groups = [[i + near * k for k in range(far)] for i in range(near)]
    near_all = [[m * owners + j for m in group for j in range(owners)] for group in near_groups]

    payload = pl.pallas_call(
        payload_body,
        out_shape=jax.ShapeDtypeStruct((heads, 3 * tokens + 8, lanes), BF16),
        in_specs=[pl.BlockSpec(memory_space=pl.ANY)] * 4,
        out_specs=whole(1)[0],
        scratch_shapes=[
            *[pltpu.VMEM((tokens, columns), BF16)] * 3,
            pltpu.VMEM((heads, tokens), F32),
            pltpu.SemaphoreType.DMA((4,)),
        ],
        name="payload",
    )(queries, key_rows, value_rows, jnp.transpose(decay_log))
    arrived = lax.all_to_all(payload, "seq", 0, 0, tiled=True, axis_index_groups=near_groups)
    span = near * tokens
    query = arrived[:, :tokens].reshape(span, lanes)
    key = arrived[:, tokens : 2 * tokens].reshape(span, lanes)
    value = arrived[:, 2 * tokens : 3 * tokens].reshape(span, lanes)
    within = arrived[:, 3 * tokens : 3 * tokens + 3, :tokens].astype(F32).sum(axis=1)
    ends = within[:, -1]
    starts = jnp.cumsum(ends) - ends
    cum = (within + starts[:, None]).reshape(span)
    state, fade, own = pl.pallas_call(
        partial(state_body, tokens),
        out_shape=(
            jax.ShapeDtypeStruct((lanes, lanes), F32),
            jax.ShapeDtypeStruct((8, lanes), F32),
            jax.ShapeDtypeStruct((lanes + 8, lanes), BF16),
        ),
        in_specs=whole(1),
        out_specs=tuple(whole(3)),
        compiler_params=SMALL,
        name="group_state",
    )(arrived)
    fade = fade[:1]
    my_far = lax.axis_index("seq") // near

    def passed(x, pairs):
        return lax.ppermute(
            x, "seq", [(near * p + i, near * q + i) for p, q in pairs for i in range(near)]
        )

    order = sorted(range(1, far), key=lambda g: (g != 1, min(g, far - g), -g))
    from_zero = jnp.zeros((lanes + 8, lanes), F32)
    from_one = jnp.zeros((lanes + 8, lanes), F32)
    direct = []
    for g in order:
        other = g + 1 if g < far - 1 else 2
        pairs = [(0, g)] if g == 1 else [(0, g), (1, other)]
        direct.append((g, passed(own, pairs)))
    scales = jnp.exp2(jnp.arange(8, dtype=F32) / 8)[:, None]
    scales = jnp.broadcast_to(scales, (8, lanes))
    offset = jnp.pad(state, ((0, 8), (0, 0)))
    carried = jnp.pad(jnp.where(my_far <= 2, scales, 0.0), ((lanes, 0), (0, 0)))
    for k in range(2, far - 1):
        running = (fade * carried + offset).astype(BF16)
        received = passed(running, [(k, k + 1)])
        carried = carried + received.astype(F32)
    after_one = jnp.mean(carried[lanes:] / scales, axis=0)
    for g, x in direct:
        x = x.astype(F32)
        from_zero = from_zero + jnp.where(my_far == g, x, 0.0)
        from_one = from_one + jnp.where(my_far == g, 0.0, x)
    one = from_one[lanes] + from_one[lanes + 1] + from_one[lanes + 2]
    after_zero = after_one * jnp.where(my_far >= 2, one, 1.0)
    incoming = carried[:lanes] + after_one * from_one[:lanes] + after_zero * from_zero[:lanes]
    scores = lax.dot_general(query, key, (((1,), (1,)), ((), ())), preferred_element_type=F32)
    places = jnp.arange(span)
    causal = places[:, None] >= places[None, :]
    decays = jnp.where(causal, jnp.exp(jnp.where(causal, cum[:, None] - cum[None, :], 0.0)), 0.0)
    mixing = (scores * decays).astype(BF16)
    lifted = (query.astype(F32) * jnp.exp(cum)[:, None]).astype(BF16)
    local_part = lax.optimization_barrier(
        jnp.dot(mixing, value, preferred_element_type=F32)
    )
    attended = local_part + jnp.dot(lifted, incoming.astype(BF16), preferred_element_type=F32)
    attended = attended.astype(BF16).reshape(near, tokens, lanes)
    attended = lax.all_to_all(attended, "seq", 0, 0, tiled=True, axis_index_groups=near_groups)
    attended = jnp.swapaxes(attended, 0, 1).reshape(tokens, columns).astype(F32)

    sumsq = jnp.sum(attended * attended, axis=1)
    branch = jax.nn.sigmoid(out_gate.astype(F32)) * attended * attn_gain
    dispatch, combine = slot_tables(routes, route_weights, experts, CAP)
    both = jnp.concatenate([residual, branch.astype(BF16)], axis=1)
    packed = jnp.dot(jnp.transpose(dispatch).astype(BF16), both, preferred_element_type=F32)
    packed = packed.astype(BF16).reshape(owners, half_cap * 2 * heads, lanes)
    sums = jnp.pad(three_terms(sumsq), ((0, 0), (0, lanes - tokens)))
    gains = three_terms(moe_gain).reshape(3 * heads, lanes)
    extra = jnp.concatenate([sums, gains], axis=0)
    extra = padded_rows(extra, 16)
    extra = jnp.broadcast_to(extra[None], (owners, *extra.shape))
    payload = jnp.concatenate([packed, extra], axis=1)
    arrived = lax.all_to_all(payload, ("exp", "rep"), 0, 0, tiled=True)
    size = half_cap * 2 * heads
    rows = arrived[:, :size].reshape(owners, half_cap, 2, columns).astype(F32)
    sums = arrived[:, size : size + 3, :tokens].astype(F32).sum(axis=(0, 1))
    gains = arrived[:, size + 3 : size + 3 + 3 * heads].astype(F32)
    gains = gains.reshape(owners, 3, columns).sum(axis=1)
    attn_scale = lax.rsqrt(sums / width + EPSILON)
    me = lax.axis_index(("exp", "rep"))
    mine = lax.dynamic_slice_in_dim(dispatch, me * half_cap, half_cap, axis=1)
    slot_scale = jnp.sum(mine * attn_scale[:, None], axis=0)
    slot_hidden = rows[:, :, 0] + slot_scale[None, :, None] * rows[:, :, 1]
    moe_sumsq = jnp.sum(slot_hidden * slot_hidden, axis=(0, 2))
    moe_scale = lax.rsqrt(moe_sumsq / width + EPSILON)
    normed = (slot_hidden * moe_scale[None, :, None] * gains[:, None, :]).astype(BF16)
    normed = jnp.swapaxes(normed, 0, 1).reshape(half_cap * width // lanes, lanes)

    gathered = lax.all_gather(normed, "seq", axis=0, tiled=True, axis_index_groups=far_groups)
    gathered = lax.all_gather(gathered, "seq", axis=0, tiled=True, axis_index_groups=near_groups)
    slot_rows = gathered.reshape(blocks * half_cap, width)
    pieces = pl.pallas_call(
        partial(expert_body, near),
        out_shape=jax.ShapeDtypeStruct((near * owners, far * half_cap, columns), BF16),
        in_specs=[*whole(3), pl.BlockSpec(memory_space=pl.ANY)],
        out_specs=whole(1)[0],
        scratch_shapes=[pltpu.VMEM(w_down.shape, BF16), pltpu.SemaphoreType.DMA],
        compiler_params=pltpu.CompilerParams(vmem_limit_bytes=52_500_000),
        name="experts",
    )(slot_rows, w_gate, w_up, w_down)
    pieces = lax.all_to_all(
        pieces, ("seq", "exp", "rep"), 0, 0, tiled=True, axis_index_groups=near_all
    )
    pieces = pieces.reshape(near, owners, far, half_cap, columns).astype(F32).sum(axis=0)
    pieces = jnp.swapaxes(pieces.astype(BF16), 0, 1).reshape(far, owners * half_cap, columns)
    pieces = lax.all_to_all(pieces, "seq", 0, 0, tiled=True, axis_index_groups=far_groups)
    returned = pieces.astype(F32).sum(axis=0).astype(BF16)
    expert_mix = jnp.dot(combine, returned.astype(F32), precision=lax.Precision.HIGHEST)
    hidden = residual.astype(F32) + attn_scale[:, None] * branch
    return (hidden + expert_mix).astype(BF16)


def solution(mesh):
    return jax.shard_map(
        shards,
        mesh=mesh,
        in_specs=(
            P(("groups", "seq"), ("exp", "rep")),
            P(("groups", "seq"), ("exp", "rep")),
            P(("groups", "seq"), ("exp", "rep")),
            P(("groups", "seq"), ("exp", "rep")),
            P(("groups", "seq"), ("exp", "rep")),
            P(("groups", "seq"), ("exp", "rep")),
            P(("exp", "rep")),
            P(("exp", "rep")),
            P(("groups", "seq"), None),
            P(("groups", "seq"), None),
            P("exp", "seq", None),
            P("exp", "seq", None),
            P("exp", "seq", None),
        ),
        out_specs=P(("groups", "seq"), ("exp", "rep")),
        check_vma=False,
    )
```

```python
from functools import partial

import jax
import jax.numpy as jnp
from jax import lax
from jax.experimental import pallas as pl
from jax.experimental.pallas import tpu as pltpu
from jax.sharding import PartitionSpec as P

CAP = 6


EPSILON = 1e-06

F32 = jnp.float32
BF16 = jnp.bfloat16


def three_terms(x):
    high = lax.reduce_precision(x, 8, 7)
    rest = x - high
    middle = lax.reduce_precision(rest, 8, 7)
    low = rest - middle
    return jnp.stack([high, middle, low]).astype(BF16)


def slot_tables(route_block, weight_block, experts, capacity):
    expert_ids = jnp.arange(experts, dtype=jnp.int32)
    onehot = (route_block[:, :, None] == expert_ids[None, None, :]).astype(jnp.int32)
    tokens = route_block.shape[0]
    flat_hits = onehot.reshape(tokens * 2, experts)
    before = jnp.cumsum(flat_hits, axis=0) - flat_hits
    places = jnp.arange(capacity, dtype=jnp.int32)
    hit_table = flat_hits[:, :, None] * (before[:, :, None] == places[None, None, :]).astype(
        jnp.int32
    )
    hit_table = hit_table.astype(jnp.float32).reshape(tokens, 2, experts * capacity)
    dispatch = jnp.sum(hit_table, axis=1)
    combine = jnp.sum(hit_table * weight_block[:, :, None], axis=1)
    return (dispatch, combine)


def padded_rows(x, rows):
    return jnp.pad(x, [(0, 0)] * (x.ndim - 2) + [(0, rows - x.shape[-2]), (0, 0)])


def rounded(x):
    return x.astype(BF16).astype(F32)


def payload_body(
    query_hbm, key_hbm, value_hbm, decay_hbm, out_ref, query_ref, key_ref, value_ref, decay_ref, arrivals
):
    fetches = [
        pltpu.make_async_copy(source, target, arrivals.at[i])
        for i, (source, target) in enumerate(
            [
                (decay_hbm, decay_ref),
                (query_hbm, query_ref),
                (key_hbm, key_ref),
                (value_hbm, value_ref),
            ]
        )
    ]
    for fetch in fetches:
        fetch.start()
    tokens, columns = query_ref.shape
    heads = out_ref.shape[0]
    lanes = columns // heads
    row = lax.broadcasted_iota(jnp.int32, (tokens, lanes), 0)
    col = lax.broadcasted_iota(jnp.int32, (tokens, lanes), 1)
    upto = jnp.where((row <= col) & (col < tokens), 1.0, 0.0)
    fetches[0].wait()
    cumulative = jnp.dot(
        decay_ref[...], upto, precision=lax.Precision.HIGHEST, preferred_element_type=F32
    )
    high = rounded(cumulative)
    middle = rounded(cumulative - high)
    low = cumulative - high - middle
    place = lax.broadcasted_iota(jnp.int32, (8, lanes), 0)
    for fetch in fetches[1:]:
        fetch.wait()
    for h in range(heads):
        here = slice(h * lanes, (h + 1) * lanes)
        out_ref[h, :tokens] = query_ref[:, here]
        out_ref[h, tokens : 2 * tokens] = key_ref[:, here]
        out_ref[h, 2 * tokens : 3 * tokens] = value_ref[:, here]
        tail = jnp.where(place == 0, high[h : h + 1], 0.0)
        tail = jnp.where(place == 1, middle[h : h + 1], tail)
        tail = jnp.where(place == 2, low[h : h + 1], tail)
        out_ref[h, 3 * tokens :] = tail.astype(BF16)


def state_body(tokens, arrived_ref, state_ref, fade_ref):
    near, _, lanes = arrived_ref.shape
    sums = [
        jnp.sum(arrived_ref[b, 3 * tokens :].astype(F32), axis=0, keepdims=True)
        for b in range(near)
    ]
    ends = [x[:, tokens - 1 : tokens] for x in sums]
    left = jnp.zeros_like(ends[0])
    state = jnp.zeros((lanes, lanes), F32)
    for b in reversed(range(near)):
        left = left + ends[b]
        weight = jnp.exp(left - sums[b][:, :tokens])
        key = jnp.transpose(arrived_ref[b, tokens : 2 * tokens].astype(F32))
        state = state + jnp.dot(
            (key * weight).astype(BF16),
            arrived_ref[b, 2 * tokens : 3 * tokens],
            preferred_element_type=F32,
        )
    state_ref[...] = state
    fade_ref[...] = jnp.broadcast_to(jnp.exp(left), fade_ref.shape)


def expert_body(
    near, rows_ref, gate_ref, up_hbm, down_hbm, out_ref, up_ref, down_ref, arrivals
):
    pieces, height, columns = out_ref.shape
    fetches = [
        pltpu.make_async_copy(up_hbm, up_ref, arrivals.at[0]),
        pltpu.make_async_copy(down_hbm, down_ref, arrivals.at[1]),
    ]
    for fetch in fetches:
        fetch.start()
    owners = pieces // near
    contract = (((1,), (1,)), ((), ()))
    rows = rows_ref[...]
    gate = lax.dot_general(rows, gate_ref[0], contract, preferred_element_type=F32)
    fetches[0].wait()
    up = lax.dot_general(rows, up_ref[0], contract, preferred_element_type=F32)
    inner = (gate / (1.0 + jnp.exp(-gate)) * up).astype(BF16)
    fetches[1].wait()
    for j in range(owners):
        part = jnp.dot(
            inner,
            down_ref[0, :, j * columns : (j + 1) * columns],
            preferred_element_type=F32,
        ).astype(BF16)
        for r in range(near):
            out_ref[r * owners + j] = part[r * height : (r + 1) * height]


SMALL = pltpu.CompilerParams(vmem_limit_bytes=4 * 1024 * 1024)


def whole(count):
    return [pl.BlockSpec(memory_space=pltpu.VMEM)] * count


def shards(
    queries,
    key_rows,
    value_rows,
    decay_log,
    residual,
    out_gate,
    attn_gain,
    moe_gain,
    routes,
    route_weights,
    w_gate,
    w_up,
    w_down,
):
    tokens, columns = queries.shape
    heads = decay_log.shape[1]
    lanes = columns // heads
    blocks = lax.axis_size("seq")
    near = heads
    far = blocks // near
    experts = lax.axis_size("exp")
    copies = lax.axis_size("rep")
    owners = experts * copies
    width = columns * owners
    half_cap = CAP // copies
    near_groups = [[near * i + k for k in range(near)] for i in range(far)]
    far_groups = [[i + near * k for k in range(far)] for i in range(near)]
    near_all = [[m * owners + j for m in group for j in range(owners)] for group in near_groups]

    payload = pl.pallas_call(
        payload_body,
        out_shape=jax.ShapeDtypeStruct((heads, 3 * tokens + 8, lanes), BF16),
        in_specs=[pl.BlockSpec(memory_space=pl.ANY)] * 4,
        out_specs=whole(1)[0],
        scratch_shapes=[
            *[pltpu.VMEM((tokens, columns), BF16)] * 3,
            pltpu.VMEM((heads, tokens), F32),
            pltpu.SemaphoreType.DMA((4,)),
        ],
        name="payload",
    )(queries, key_rows, value_rows, jnp.transpose(decay_log))
    arrived = lax.all_to_all(payload, "seq", 0, 0, tiled=True, axis_index_groups=near_groups)
    span = near * tokens
    query = arrived[:, :tokens].reshape(span, lanes)
    key = arrived[:, tokens : 2 * tokens].reshape(span, lanes)
    value = arrived[:, 2 * tokens : 3 * tokens].reshape(span, lanes)
    within = arrived[:, 3 * tokens : 3 * tokens + 3, :tokens].astype(F32).sum(axis=1)
    ends = within[:, -1]
    starts = jnp.cumsum(ends) - ends
    cum = (within + starts[:, None]).reshape(span)
    state, fade = pl.pallas_call(
        partial(state_body, tokens),
        out_shape=(
            jax.ShapeDtypeStruct((lanes, lanes), F32),
            jax.ShapeDtypeStruct((8, lanes), F32),
        ),
        in_specs=whole(1),
        out_specs=tuple(whole(2)),
        compiler_params=SMALL,
        name="group_state",
    )(arrived)
    fade = fade[:1]
    my_far = lax.axis_index("seq") // near
    first = state.astype(BF16)
    order = sorted(range(1, far), key=lambda g: (g != 1, min(g, far - g), -g))
    from_first = []
    for g in order:
        from_first.append(
            lax.ppermute(first, "seq", [(i, near * g + i) for i in range(near)])
        )
    scales = jnp.exp2(jnp.arange(8, dtype=F32) / 8)[:, None]
    scales = jnp.broadcast_to(scales, (8, lanes))
    own = jnp.pad(state, ((0, 8), (0, 0)))
    opening = jnp.where(my_far <= 1, scales, 0.0)
    carried = jnp.pad(opening, ((lanes, 0), (0, 0)))
    for k in range(1, far - 1):
        running = (fade * carried + own).astype(BF16)
        passed = [(near * k + i, near * (k + 1) + i) for i in range(near)]
        received = lax.ppermute(running, "seq", passed)
        carried = carried + received.astype(F32)
    factor = jnp.mean(carried[lanes:] / scales, axis=0)
    from_first = sum(x.astype(F32) for x in from_first)
    incoming = carried[:lanes] + factor * from_first
    scores = lax.dot_general(query, key, (((1,), (1,)), ((), ())), preferred_element_type=F32)
    places = jnp.arange(span)
    causal = places[:, None] >= places[None, :]
    decays = jnp.where(causal, jnp.exp(jnp.where(causal, cum[:, None] - cum[None, :], 0.0)), 0.0)
    mixing = (scores * decays).astype(BF16)
    lifted = (query.astype(F32) * jnp.exp(cum)[:, None]).astype(BF16)
    local_part = lax.optimization_barrier(
        jnp.dot(mixing, value, preferred_element_type=F32)
    )
    attended = local_part + jnp.dot(lifted, incoming.astype(BF16), preferred_element_type=F32)
    attended = attended.astype(BF16).reshape(near, tokens, lanes)
    attended = lax.all_to_all(attended, "seq", 0, 0, tiled=True, axis_index_groups=near_groups)
    attended = jnp.swapaxes(attended, 0, 1).reshape(tokens, columns).astype(F32)

    sumsq = jnp.sum(attended * attended, axis=1)
    branch = jax.nn.sigmoid(out_gate.astype(F32)) * attended * attn_gain
    dispatch, combine = slot_tables(routes, route_weights, experts, CAP)
    both = jnp.concatenate([residual, branch.astype(BF16)], axis=1)
    packed = jnp.dot(jnp.transpose(dispatch).astype(BF16), both, preferred_element_type=F32)
    packed = packed.astype(BF16).reshape(owners, half_cap * 2 * heads, lanes)
    sums = jnp.pad(three_terms(sumsq), ((0, 0), (0, lanes - tokens)))
    gains = three_terms(moe_gain).reshape(3 * heads, lanes)
    extra = jnp.concatenate([sums, gains], axis=0)
    extra = padded_rows(extra, 16)
    extra = jnp.broadcast_to(extra[None], (owners, *extra.shape))
    payload = jnp.concatenate([packed, extra], axis=1)
    arrived = lax.all_to_all(payload, ("exp", "rep"), 0, 0, tiled=True)
    size = half_cap * 2 * heads
    rows = arrived[:, :size].reshape(owners, half_cap, 2, columns).astype(F32)
    sums = arrived[:, size : size + 3, :tokens].astype(F32).sum(axis=(0, 1))
    gains = arrived[:, size + 3 : size + 3 + 3 * heads].astype(F32)
    gains = gains.reshape(owners, 3, columns).sum(axis=1)
    attn_scale = lax.rsqrt(sums / width + EPSILON)
    me = lax.axis_index(("exp", "rep"))
    mine = lax.dynamic_slice_in_dim(dispatch, me * half_cap, half_cap, axis=1)
    slot_scale = jnp.sum(mine * attn_scale[:, None], axis=0)
    slot_hidden = rows[:, :, 0] + slot_scale[None, :, None] * rows[:, :, 1]
    moe_sumsq = jnp.sum(slot_hidden * slot_hidden, axis=(0, 2))
    moe_scale = lax.rsqrt(moe_sumsq / width + EPSILON)
    normed = (slot_hidden * moe_scale[None, :, None] * gains[:, None, :]).astype(BF16)
    normed = jnp.swapaxes(normed, 0, 1).reshape(half_cap * width // lanes, lanes)

    gathered = lax.all_gather(normed, "seq", axis=0, tiled=True, axis_index_groups=far_groups)
    gathered = lax.all_gather(gathered, "seq", axis=0, tiled=True, axis_index_groups=near_groups)
    slot_rows = gathered.reshape(blocks * half_cap, width)
    pieces = pl.pallas_call(
        partial(expert_body, near),
        out_shape=jax.ShapeDtypeStruct((near * owners, far * half_cap, columns), BF16),
        in_specs=[*whole(2), *[pl.BlockSpec(memory_space=pl.ANY)] * 2],
        out_specs=whole(1)[0],
        scratch_shapes=[
            *[pltpu.VMEM(w.shape, BF16) for w in (w_up, w_down)],
            pltpu.SemaphoreType.DMA((2,)),
        ],
        compiler_params=pltpu.CompilerParams(vmem_limit_bytes=53_200_000),
        name="experts",
    )(slot_rows, w_gate, w_up, w_down)
    pieces = lax.all_to_all(
        pieces, ("seq", "exp", "rep"), 0, 0, tiled=True, axis_index_groups=near_all
    )
    pieces = pieces.reshape(near, owners, far, half_cap, columns).astype(F32).sum(axis=0)
    pieces = jnp.swapaxes(pieces.astype(BF16), 0, 1).reshape(far, owners * half_cap, columns)
    pieces = lax.all_to_all(pieces, "seq", 0, 0, tiled=True, axis_index_groups=far_groups)
    returned = pieces.astype(F32).sum(axis=0).astype(BF16)
    expert_mix = jnp.dot(combine, returned.astype(F32), precision=lax.Precision.HIGHEST)
    hidden = residual.astype(F32) + attn_scale[:, None] * branch
    return (hidden + expert_mix).astype(BF16)


def solution(mesh):
    return jax.shard_map(
        shards,
        mesh=mesh,
        in_specs=(
            P(("groups", "seq"), ("exp", "rep")),
            P(("groups", "seq"), ("exp", "rep")),
            P(("groups", "seq"), ("exp", "rep")),
            P(("groups", "seq"), ("exp", "rep")),
            P(("groups", "seq"), ("exp", "rep")),
            P(("groups", "seq"), ("exp", "rep")),
            P(("exp", "rep")),
            P(("exp", "rep")),
            P(("groups", "seq"), None),
            P(("groups", "seq"), None),
            P("exp", "seq", None),
            P("exp", "seq", None),
            P("exp", "seq", None),
        ),
        out_specs=P(("groups", "seq"), ("exp", "rep")),
        check_vma=False,
    )
```
